32 devices in a mesh: tm: 4 (over z), mem: 4 (over y, x), tile: 2 (over core).
Axes of the slice: x: 2, y: 2, z: 4, core: 2. Of those that a mesh axis runs over, the one named last changes fastest.
Arguments:
- control: float32 [40, 2, 8, 256], P('mem', None, 'tile'), may hold values from -6 to 6
- vertical_modes: float32 [64, 2], replicated, may hold values from -4 to 4
- mode_counts: int32 [8], P('tile'), may hold values from 1 to 2, as said below
- perturbations: bfloat16 [40, 8, 64, 8, 256], P('mem', 'tm', None, 'tile'), may hold values from -6 to 6
- slot_index: int32 [12], P('tm'), may hold values from 0 to 7, as said below
- blend_weight: float32 [12], P('tm'), may hold values from 0 to 1
Outputs:
- increment: float32 [12, 64, 8, 256], P('tm', None, 'tile')
The draws below stay inside these ranges and needn't reach their ends.
Inputs may be any that keep to these rules, and one draw needn't show every extreme that they name: slot_index[w] // 2 == w // 3. `mode_counts`: both ends of the range occur.
All inputs are finite; a program needn't handle non-finite values.
Results may differ from the reference program's by a relative error of at most 0.0003.
Values sent between devices are 32-bit elements; how exact they have to be, the bound alone decides.
A program may use at most 64 MiB of HBM per device.

```python
import math
import jax
import jax.numpy as jnp
from jax import lax

LEV = 64
VM = 2
SMOOTH = 4
SLOT_DEV = 2
WIN_DEV = 3
GY = 256
ENS = 40
SLOTS = 8
WIN = 12
NX = 8


def draw_slot_index(key, part):
    blocks = jnp.arange(WIN) // WIN_DEV
    offsets = jax.random.randint(key, (WIN,), 0, SLOT_DEV)
    return (blocks * SLOT_DEV + offsets).astype(jnp.int32)


def draw_mode_counts(key, part):
    first_key = jax.random.fold_in(key, 11)
    second_key = jax.random.fold_in(key, 23)
    counts = jax.random.randint(first_key, (NX,), 1, VM + 1)
    where = jax.random.randint(second_key, (), 0, NX)
    counts = counts.at[where].set(1)
    counts = counts.at[(where + 1) % NX].set(VM)
    return counts.astype(jnp.int32)


def block_scale(stream_key, dims, pieces, smallest, largest):
    gain, own = 1.0, jax.random.fold_in(stream_key, 6)
    for position, parts in pieces:
        steps = jnp.exp(jax.random.uniform(jax.random.fold_in(own, position), (parts,), jnp.float32, smallest / len(pieces), largest / len(pieces)))
        gain = gain * jnp.repeat(steps, dims[position] // parts).reshape([-1 if axis == position else 1 for axis in range(len(dims))])
    return gain


def bell_draw(rng, shape, scale, bound, pieces=(), held_as=jnp.bfloat16):
    array = scale * jax.random.normal(rng, shape, jnp.float32)
    if pieces:
        array = array * block_scale(rng, shape, pieces, -0.22, 0.18)
    return jnp.clip(array, -bound, bound).astype(held_as)


def setup_inputs(seed: int = 0) -> dict:
    splits = jax.random.split(jax.random.key(seed), 7)
    control = bell_draw(splits[0], (ENS, VM, NX, GY), 1.0, 6.0, ((0, 4), (2, 2)), jnp.float32)
    vertical_modes = bell_draw(splits[1], (LEV, VM), 1.0, 4.0, (), jnp.float32)
    mode_counts = draw_mode_counts(jax.random.fold_in(splits[6], 71), 0)
    perturbations = bell_draw(splits[3], (ENS, SLOTS, LEV, NX, GY), 1.0, 6.0, ((0, 4), (1, 4), (3, 2)))
    slot_index = draw_slot_index(jax.random.fold_in(splits[6], 71), 0)
    blend_weight = jnp.clip(1.0 * jax.random.uniform(splits[5], (WIN,), jnp.float32) ** block_scale(splits[5], (WIN,), ((0, 4),), -0.2, 0.2), 0.0, 1.0)
    return dict(control=control, vertical_modes=vertical_modes, mode_counts=mode_counts, perturbations=perturbations, slot_index=slot_index, blend_weight=blend_weight)


diffusion = 0.24

def relax_global(field):
    neighbours = jnp.roll(field, -1, axis=2) + jnp.roll(field, 1, axis=2)
    padded = jnp.pad(field, ((0, 0), (0, 0), (0, 0), (1, 1)))
    lateral = padded[:, :, :, 2:] + padded[:, :, :, :-2]
    return field + diffusion * (neighbours + lateral - 4.0 * field)

def reference(control, vertical_modes, mode_counts, perturbations, slot_index, blend_weight):
    smoothed = control
    for repeat in range(SMOOTH):
        smoothed = relax_global(smoothed)
    localized = jnp.zeros((ENS, LEV, NX, GY), jnp.float32)
    for mode_index in range(VM):
        keep_mode = (mode_index < mode_counts).astype(jnp.float32)
        masked = keep_mode[None, :, None] * smoothed[:, mode_index]
        localized = localized + vertical_modes[:, mode_index][None, :, None, None] * masked[:, None]
    norm_factor = 1.0 / math.sqrt(ENS - 1)
    slots = []
    for slot in range(SLOTS):
        member_total = lax.optimization_barrier(jnp.sum(localized * perturbations[:, slot].astype(jnp.float32), axis=0))
        slots.append(member_total * norm_factor)
    slot_increment = jnp.stack(slots)
    cumulative = jnp.cumsum(slot_increment, axis=0)
    previous = jnp.concatenate([jnp.zeros((1, LEV, NX, GY), jnp.float32), cumulative[:-1]], axis=0)
    weight = blend_weight[:, None, None, None]
    return weight * cumulative[slot_index] + (1.0 - weight) * previous[slot_index]
```

```python
import functools
import math

import jax
import jax.numpy as jnp
from jax import lax
from jax.experimental import pallas as pl
from jax.experimental.pallas import tpu as pltpu
from jax.sharding import PartitionSpec as P

SMOOTH = 4
CHUNKS = 4
DIRECT = (1,)
PIECES = 4
LANES = 128
MESH = pl.DeviceIdType.MESH

diffusion = 0.24


def drain(ref, sem):
    pltpu.make_async_copy(ref, ref, sem).wait()


def kernel(dims, control, perturbations, modes_in, counts_in, ext, own, near, away, pert, smooth, part,
           first_a, first_b, mid_a, mid_b, second_a, second_b, passing, modes, counts,
           load_sem, halo_send, halo_recv, rs_send, rs_recv, z_send, z_recv, ag_send, hop_recv, end_recv):
    members, slots, modes_n, nx, halves, outer, inner, rows, tiles, steps_tm, norm = dims
    tm = lax.axis_index("tm")
    mem = lax.axis_index("mem")
    tile = lax.axis_index("tile")
    jy, ix = mem // inner, mem % inner
    level_rows = nx * halves
    part_levels = rows // level_rows

    def inner_peer(d):
        return (ix + d) % inner

    def outer_peer(d):
        return (jy + d) % outer

    def at(j, i):
        return {"mem": j * inner + i}

    barrier = pltpu.get_barrier_semaphore()
    tile_offsets = sorted({1 % tiles, (tiles - 1) % tiles} - {0})
    expected = len(tile_offsets) + inner - 1 + outer - 1
    for d in tile_offsets:
        pl.semaphore_signal(barrier, inc=1, device_id={"tile": (tile + d) % tiles}, device_id_type=MESH)
    for d in range(1, inner):
        pl.semaphore_signal(barrier, inc=1, device_id=at(jy, inner_peer(d)), device_id_type=MESH)
    for e in range(1, outer):
        pl.semaphore_signal(barrier, inc=1, device_id=at(outer_peer(e), ix), device_id_type=MESH)

    @pl.when(tm > 0)
    def _():
        pl.semaphore_signal(barrier, inc=1, device_id={"tm": tm - 1}, device_id_type=MESH)

    @pl.when(tm < steps_tm - 1)
    def _():
        pl.semaphore_signal(barrier, inc=1, device_id={"tm": tm + 1}, device_id_type=MESH)

    load_own = pltpu.make_async_copy(control, own, load_sem.at[0])
    load_own.start()
    load_counts = pltpu.make_async_copy(counts_in, counts, load_sem.at[1])
    load_counts.start()
    load_modes = pltpu.make_async_copy(modes_in, modes, load_sem.at[2])
    load_modes.start()

    def load(o, j, i, sem):
        span = pl.ds(o * CHUNKS, CHUNKS)
        pltpu.make_async_copy(
            perturbations.at[:, :, j, i, span], pert.at[:, :, j, i, span], load_sem.at[sem]).start()

    def loaded(o, j, i, sem):
        drain(pert.at[:, :, j, i, pl.ds(o * CHUNKS, CHUNKS)], load_sem.at[sem])

    every = slice(None)
    groups = []
    for d in range(1, inner):
        groups.append((0, every, inner_peer(d)))
        for e in range(1, outer + 1):
            load(0, outer_peer(e), inner_peer(d), 2 + len(groups))
    for e in range(1, outer):
        groups.append((1, outer_peer(e), every))
        for d in range(1, inner + 1):
            load(1, outer_peer(e), inner_peer(d), 2 + len(groups))
    n_first = len(groups)
    groups.append((0, every, ix))
    for e in range(1, outer + 1):
        load(0, outer_peer(e), ix, 2 + len(groups))
    groups.append((1, jy, every))
    for d in range(1, inner + 1):
        load(1, jy, inner_peer(d), 2 + len(groups))

    row = lax.broadcasted_iota(jnp.int32, (1, level_rows, LANES), 1)
    lane = lax.broadcasted_iota(jnp.int32, (1, level_rows, LANES), 2)
    lon, half = row % nx, row // nx
    first_lon, last_lon = lon == 0, lon == nx - 1
    first_lane, last_lane = lane == 0, lane == LANES - 1
    has_next, has_prev = half < halves - 1, half > 0
    back = level_rows - 1

    def after(v):
        return pltpu.roll(v, level_rows - nx, 1)

    def before(v):
        return after(v) if halves == 2 else pltpu.roll(v, nx, 1)

    def spread(left, right):
        east = pltpu.roll(jnp.where(first_lon, before(right), 0.0), back, 1)
        west = pltpu.roll(jnp.where(last_lon, after(left), 0.0), 1, 1)
        return diffusion * (east + west)

    def relax(left, v, right):
        ahead, behind = after(v), before(v)
        east = pltpu.roll(jnp.where(first_lon, before(right), v), back, 1)
        west = pltpu.roll(jnp.where(last_lon, after(left), v), 1, 1)
        up = pltpu.roll(jnp.where(first_lane, jnp.where(has_next, ahead, 0.0), v), LANES - 1, 2)
        down = pltpu.roll(jnp.where(last_lane, jnp.where(has_prev, behind, 0.0), v), 1, 2)
        return (1.0 - 4.0 * diffusion) * v + diffusion * ((east + west) + (up + down))

    fields = own.shape[0]
    batch = fields // 2 if fields % 2 == 0 and (fields // 2) % modes_n == 0 else fields

    load_own.wait()
    zero = jnp.zeros((1, level_rows, LANES), jnp.float32)

    def smooth_batch(b, carry):
        span = pl.ds(b * batch, batch)
        c = own[span]
        if tiles == 1:
            for _ in range(SMOOTH):
                c = relax(c, c, c)
        elif tiles == 2:
            c, o = relax(zero, c, zero), spread(c, c)
            for _ in range(1, SMOOTH):
                c, o = relax(o, c, o), relax(c, o, c)
            away[0, span] = o
        else:
            c, left, right = relax(zero, c, zero), spread(zero, c), spread(c, zero)
            for _ in range(1, SMOOTH):
                c, left, right = relax(left, c, right), relax(zero, left, c), relax(c, right, zero)
            away[0, span] = right
            away[1, span] = left
        smooth[span] = c
        return carry

    lax.fori_loop(0, fields // batch, smooth_batch, 0)

    chain_peers = jnp.where(tm > 0, 1, 0) + jnp.where(tm < steps_tm - 1, 1, 0)
    pl.semaphore_wait(barrier, expected + chain_peers)

    halos = []
    for n, d in enumerate(tile_offsets):
        copy = pltpu.make_async_remote_copy(
            src_ref=away.at[n], dst_ref=near.at[n], send_sem=halo_send.at[n], recv_sem=halo_recv.at[n],
            device_id={"tile": (tile + d) % tiles}, device_id_type=MESH)
        copy.start()
        halos.append(copy)

    load_counts.wait()
    load_modes.wait()
    count = jnp.zeros((1, level_rows, LANES), jnp.int32)
    for x in range(nx):
        count = jnp.where(lon == x, counts[x], count)
    for copy in halos:
        copy.wait_recv()
    total = smooth[...]
    for n in range(len(tile_offsets)):
        total = total + near[n]
    mode = lax.broadcasted_iota(jnp.int32, (fields, level_rows, LANES), 0) % modes_n
    smooth[...] = jnp.where(mode < count, total * norm, 0.0)

    pair = 2 * level_rows

    def sums(p, j, i, u):
        base = ((j * inner + i) * 2 * CHUNKS + p) * part_levels + 2 * u
        for t in range(slots):
            acc = [[None] * 2 for _ in range(modes_n)]
            for k in range(members):
                x = pert[k, t, j, i, p, pl.ds(pl.multiple_of(u * pair, pair), pair), :].astype(jnp.float32)
                for m in range(modes_n):
                    s = smooth[k * modes_n + m]
                    for v in range(2):
                        term = s * x[v * level_rows:(v + 1) * level_rows]
                        acc[m][v] = term if k == 0 else acc[m][v] + term
            for v in range(2):
                total = modes[0, base + v] * acc[0][v]
                for m in range(1, modes_n):
                    total = total + modes[m, base + v] * acc[m][v]
                part[p, t, j, i, pl.ds(pl.multiple_of(u * pair + v * level_rows, level_rows), level_rows), :] = total

    pairs = rows // pair

    def sums_over(count, place):
        def body(n, carry):
            u, n = n % pairs, n // pairs
            sums(*place(n), u)
            return carry

        lax.fori_loop(0, count * pairs, body, 0)

    def remote(src, dst, send, recv, to):
        return pltpu.make_async_remote_copy(
            src_ref=src, dst_ref=dst, send_sem=send, recv_sem=recv, device_id=to, device_id_type=MESH)

    steps_in, steps_out = range(1, inner), range(1, outer)
    rs1, rs2 = [[], []], [[], []]
    for c in range(CHUNKS):
        pa, pb = c, CHUNKS + c
        rs1[0].append([remote(part.at[pa, :, :, inner_peer(d)], first_a.at[c, d - 1],
                              rs_send.at[0, d - 1], rs_recv.at[0, c, d - 1], at(jy, inner_peer(d)))
                       for d in steps_in])
        rs1[1].append([remote(part.at[pb, :, outer_peer(e)], first_b.at[c, e - 1],
                              rs_send.at[1, e - 1], rs_recv.at[1, c, e - 1], at(outer_peer(e), ix))
                       for e in steps_out])
        rs2[0].append([remote(mid_a.at[c, e - 1], second_a.at[c, e - 1],
                              rs_send.at[2, e - 1], rs_recv.at[2, c, e - 1], at(outer_peer(e), ix))
                       for e in steps_out])
        rs2[1].append([remote(mid_b.at[c, d - 1], second_b.at[c, d - 1],
                              rs_send.at[3, d - 1], rs_recv.at[3, c, d - 1], at(jy, inner_peer(d)))
                       for d in steps_in])

    for n, group in enumerate(groups[:n_first]):
        loaded(*group, 3 + n)
    for c in range(CHUNKS):
        for d, copy in zip(steps_in, rs1[0][c]):
            sums_over(outer, lambda n: (c, outer_peer(n), inner_peer(d)))
            copy.start()
        for e, copy in zip(steps_out, rs1[1][c]):
            sums_over(inner, lambda n: (CHUNKS + c, outer_peer(e), inner_peer(n)))
            copy.start()
    for n, group in enumerate(groups[n_first:], n_first):
        loaded(*group, 3 + n)
    sums_over(CHUNKS * outer, lambda n: (n // outer, n % outer, ix))
    sums_over(CHUNKS * inner, lambda n: (CHUNKS + n // inner, jy, n % inner))

    for c in range(CHUNKS):
        for copy in rs1[0][c]:
            copy.wait_recv()
        for e, copy in zip(steps_out, rs2[0][c]):
            total = part[c, :, outer_peer(e), ix]
            for d in steps_in:
                total = total + first_a[c, d - 1, :, outer_peer(e)]
            mid_a[c, e - 1] = total
            copy.start()
        for copy in rs1[1][c]:
            copy.wait_recv()
        for d, copy in zip(steps_in, rs2[1][c]):
            total = part[CHUNKS + c, :, jy, inner_peer(d)]
            for e in steps_out:
                total = total + first_b[c, e - 1, :, inner_peer(d)]
            mid_b[c, d - 1] = total
            copy.start()

    def span_of(unit):
        return pl.ds(unit, slots) if unit else pl.ds(0, 1)

    def gathers(unit, p):
        sends, relays = [], []
        group = p // CHUNKS

        def move(j, i, to, kind, n):
            ref = ext.at[span_of(unit), j, i, p]
            hop = unit and kind == group
            recv = hop_recv.at[p, n] if hop else end_recv.at[unit, group if unit else 0, kind, n]
            return remote(ref, ref, ag_send.at[unit, kind, n], recv, to)

        for d in steps_in:
            sends.append((0, d, move(jy, ix, at(jy, inner_peer(d)), 0, d - 1)))
        for e in steps_out:
            sends.append((1, e, move(jy, ix, at(outer_peer(e), ix), 1, e - 1)))
        for d in steps_in:
            for e in steps_out:
                n = (d - 1) * (outer - 1) + e - 1
                if not unit:
                    sends.append((2, d, move(jy, ix, at(outer_peer(e), inner_peer(d)), 2, n)))
                elif group == 0:
                    relays.append((d, move(jy, inner_peer(inner - d), at(outer_peer(e), ix), 2, n)))
                else:
                    relays.append((e, move(outer_peer(outer - e), ix, at(jy, inner_peer(d)), 2, n)))
        return sends, relays

    parts = range(2 * CHUNKS)
    turn = [o * CHUNKS + c for c in range(CHUNKS) for o in range(2)]
    slot_gathers = [gathers(1, p) for p in parts]
    early_gathers = [gathers(0, p) for p in parts]

    def start_gather(g):
        for _, _, copy in g[0]:
            copy.start()

    def relay_gather(g, p):
        for kind, d, copy in g[0]:
            if kind == p // CHUNKS:
                copy.wait_recv()
                for dd, forward in g[1]:
                    if dd == d:
                        forward.start()

    def finish_gathers(unit):
        kinds = [(0, inner - 1), (1, outer - 1), (2, (inner - 1) * (outer - 1))]
        whole = ext.at[span_of(unit), jy, ix]
        half = ext.at[span_of(unit), jy, ix, pl.ds(0, CHUNKS)]
        for kind, count in kinds:
            for n in range(count):
                if not unit:
                    drain(whole, end_recv.at[0, 0, kind, n])
                else:
                    for group in range(2):
                        if kind != group:
                            drain(half, end_recv.at[1, group, kind, n])
        for kind, count in kinds:
            for n in range(count):
                drain(whole, ag_send.at[unit, kind, n])

    chain = [remote(passing.at[p], ext.at[0, jy, ix, p], z_send, z_recv.at[p], {"tm": tm + 1})
             for p in parts]

    def add_slots(p):
        total = ext[1, jy, ix, p]
        for t in range(1, slots):
            total = total + ext[1 + t, jy, ix, p]
        return total

    def own_total(p):
        c = p % CHUNKS
        total = part[p, :, jy, ix]
        if p < CHUNKS:
            for d in steps_in:
                total = total + first_a[c, d - 1, :, jy]
            for copy in rs2[0][c]:
                copy.wait_recv()
            for e in steps_out:
                total = total + second_a[c, e - 1]
        else:
            for e in steps_out:
                total = total + first_b[c, e - 1, :, ix]
            for copy in rs2[1][c]:
                copy.wait_recv()
            for d in steps_in:
                total = total + second_b[c, d - 1]
        ext[pl.ds(1, slots), jy, ix, p] = total

    for p in turn:
        own_total(p)

        @pl.when(tm == 0)
        def _():
            ext[0, :, :, p] = jnp.zeros(ext.shape[1:3] + ext.shape[4:], jnp.float32)
            if steps_tm > 1:
                passing[p] = add_slots(p)
                chain[p].start()

        start_gather(slot_gathers[p])

    def earlier(p):
        chain[p].wait_recv()

        @pl.when(tm < steps_tm - 1)
        def _():
            passing[p] = ext[0, jy, ix, p] + add_slots(p)
            chain[p].start()

        start_gather(early_gathers[p])

    @pl.when(tm == 1)
    def _():
        for p in turn:
            earlier(p)
            relay_gather(slot_gathers[p], p)

    @pl.when(tm != 1)
    def _():
        for p in turn:
            relay_gather(slot_gathers[p], p)

    @pl.when(tm > 1)
    def _():
        for p in turn:
            earlier(p)

    finish_gathers(1)

    @pl.when(tm > 0)
    def _():
        finish_gathers(0)

    @pl.when(tm < steps_tm - 1)
    def _():
        drain(passing, z_send)

    for copy in halos:
        copy.wait_send()
    for d in steps_in:
        drain(first_a.at[:, d - 1], rs_send.at[0, d - 1])
        drain(second_b.at[:, d - 1], rs_send.at[3, d - 1])
    for e in steps_out:
        drain(first_b.at[:, e - 1], rs_send.at[1, e - 1])
        drain(second_a.at[:, e - 1], rs_send.at[2, e - 1])


def blend(slots, ext, index, weight, out, held, sems):
    windows, total_rows, _ = out.shape
    size = total_rows // PIECES
    local = [index[w] - lax.axis_index("tm") * slots for w in range(windows)]
    shares = [[jnp.where(local[w] > t, 1.0, jnp.where(local[w] == t, weight[w], 0.0))
               for t in range(slots)] for w in range(windows)]
    copies = []
    for n in range(PIECES):
        span = pl.ds(n * size, size)
        for w in range(windows):
            total = ext[0, span]
            for t in range(slots):
                total = total + shares[w][t] * ext[1 + t, span]
            held[w, span] = total
        copy = pltpu.make_async_copy(held.at[:, span], out.at[:, span], sems.at[n])
        copy.start()
        copies.append(copy)
    for copy in copies:
        copy.wait()


def rows_view(x, nx, gy):
    lead = x.shape[:-2]
    x = x.reshape(lead + (nx, gy // LANES, LANES))
    x = jnp.swapaxes(x, -3, -2)
    return x


def per_device(control, vertical_modes, mode_counts, perturbations, slot_index, blend_weight):
    members, slots, levels, nx, gy = perturbations.shape
    modes_n = control.shape[1]
    halves = gy // LANES
    level_rows = nx * halves
    tiles, n_mem, steps_tm = lax.axis_size("tile"), lax.axis_size("mem"), lax.axis_size("tm")
    inner = 2 if n_mem % 2 == 0 else 1
    outer = n_mem // inner
    parts = 2 * CHUNKS
    rows = levels // (n_mem * parts) * level_rows
    assert nx >= SMOOTH and level_rows == 8 and rows % 16 == 0
    norm = 1.0 / math.sqrt(members * n_mem - 1)
    fields = members * modes_n
    c = rows_view(control, nx, gy).reshape(fields, level_rows, LANES)
    q = rows_view(perturbations, nx, gy).reshape(members, slots, outer, inner, parts, rows, LANES)
    dims = (members, slots, modes_n, nx, halves, outer, inner, rows, tiles, steps_tm, norm)
    f32 = jnp.float32
    n_in, n_out = max(inner - 1, 1), max(outer - 1, 1)
    n_gather = max(inner - 1, outer - 1, (inner - 1) * (outer - 1), 1)
    dma = pltpu.SemaphoreType.DMA
    ext = pl.pallas_call(
        functools.partial(kernel, dims),
        out_shape=pltpu.VMEM((slots + 1, outer, inner, parts, rows, LANES), f32),
        in_specs=[
            pl.BlockSpec(memory_space=pltpu.HBM),
            pl.BlockSpec(memory_space=pltpu.HBM),
            pl.BlockSpec(memory_space=pltpu.HBM),
            pl.BlockSpec(memory_space=pltpu.HBM),
        ],
        out_specs=pl.BlockSpec(memory_space=pltpu.VMEM),
        scratch_shapes=[
            pltpu.VMEM((fields, level_rows, LANES), f32),
            pltpu.VMEM((2, fields, level_rows, LANES), f32),
            pltpu.VMEM((2, fields, level_rows, LANES), f32),
            pltpu.VMEM(q.shape, q.dtype),
            pltpu.VMEM((fields, level_rows, LANES), f32),
            pltpu.VMEM((parts, slots, outer, inner, rows, LANES), f32),
            pltpu.VMEM((CHUNKS, n_in, slots, outer, rows, LANES), f32),
            pltpu.VMEM((CHUNKS, n_out, slots, inner, rows, LANES), f32),
            pltpu.VMEM((CHUNKS, n_out, slots, rows, LANES), f32),
            pltpu.VMEM((CHUNKS, n_in, slots, rows, LANES), f32),
            pltpu.VMEM((CHUNKS, n_out, slots, rows, LANES), f32),
            pltpu.VMEM((CHUNKS, n_in, slots, rows, LANES), f32),
            pltpu.VMEM((parts, rows, LANES), f32),
            pltpu.SMEM((modes_n, levels), f32),
            pltpu.SMEM((nx,), jnp.int32),
            dma((n_in + n_out + 5,)),
            dma((2,)),
            dma((2,)),
            dma((4, max(n_in, n_out))),
            dma((4, CHUNKS, max(n_in, n_out))),
            dma,
            dma((parts,)),
            dma((2, 3, n_gather)),
            dma((parts, max(n_in, n_out))),
            dma((2, 2, 3, n_gather)),
        ],
        compiler_params=pltpu.CompilerParams(
            collective_id=0, has_side_effects=True),
    )(c, q, vertical_modes.T, mode_counts)
    ext = ext.reshape(slots + 1, levels * level_rows, LANES)
    windows = slot_index.shape[0]
    out = pl.pallas_call(
        functools.partial(blend, slots),
        out_shape=jax.ShapeDtypeStruct((windows, levels * level_rows, LANES), f32),
        in_specs=[
            pl.BlockSpec(memory_space=pltpu.VMEM),
            pl.BlockSpec(memory_space=pltpu.SMEM),
            pl.BlockSpec(memory_space=pltpu.SMEM),
        ],
        out_specs=pl.BlockSpec(memory_space=pltpu.HBM),
        scratch_shapes=[pltpu.VMEM((windows, levels * level_rows, LANES), f32), dma((PIECES,))],
        compiler_params=pltpu.CompilerParams(vmem_limit_bytes=8 << 20),
    )(ext, slot_index, blend_weight)
    out = out.reshape(windows, levels, halves, nx, LANES)
    return jnp.swapaxes(out, 2, 3).reshape(windows, levels, nx, gy)


def solution(mesh):
    placed = (
        P("mem", None, "tile", None),
        P(),
        P("tile"),
        P("mem", "tm", None, "tile", None),
        P("tm"),
        P("tm"),
    )
    return jax.shard_map(
        per_device,
        mesh=mesh,
        in_specs=placed,
        out_specs=P("tm", None, "tile", None),
        check_vma=False,
    )
```

```python
import functools
import math

import jax
import jax.numpy as jnp
from jax import lax
from jax.experimental import pallas as pl
from jax.experimental.pallas import tpu as pltpu
from jax.sharding import PartitionSpec as P

SMOOTH = 4
CHUNKS = 4
PIECES = 4
LANES = 128
MESH = pl.DeviceIdType.MESH

diffusion = 0.24


def drain(ref, sem):
    pltpu.make_async_copy(ref, ref, sem).wait()


def kernel(dims, control, perturbations, modes_in, counts_in, ext, own, near, away, pert, smooth, part,
           first_a, first_b, mid_a, mid_b, second_a, second_b, extra, passing, modes, counts,
           load_sem, halo_send, halo_recv, rs_send, rs_recv, z_send, z_recv, ag_send, hop_recv, end_recv,
           early_send, early_recv):
    members, slots, modes_n, nx, halves, outer, inner, rows, tiles, steps_tm, norm = dims
    tm = lax.axis_index("tm")
    mem = lax.axis_index("mem")
    tile = lax.axis_index("tile")
    jy, ix = mem // inner, mem % inner
    level_rows = nx * halves
    part_levels = rows // level_rows

    def inner_peer(d):
        return (ix + d) % inner

    def outer_peer(d):
        return (jy + d) % outer

    def at(j, i):
        return {"mem": j * inner + i}

    barrier = pltpu.get_barrier_semaphore()
    tile_offsets = sorted({1 % tiles, (tiles - 1) % tiles} - {0})
    expected = len(tile_offsets) + inner - 1 + outer - 1
    for d in tile_offsets:
        pl.semaphore_signal(barrier, inc=1, device_id={"tile": (tile + d) % tiles}, device_id_type=MESH)
    for d in range(1, inner):
        pl.semaphore_signal(barrier, inc=1, device_id=at(jy, inner_peer(d)), device_id_type=MESH)
    for e in range(1, outer):
        pl.semaphore_signal(barrier, inc=1, device_id=at(outer_peer(e), ix), device_id_type=MESH)

    @pl.when(tm > 0)
    def _():
        pl.semaphore_signal(barrier, inc=1, device_id={"tm": tm - 1}, device_id_type=MESH)

    @pl.when(tm < steps_tm - 1)
    def _():
        pl.semaphore_signal(barrier, inc=1, device_id={"tm": tm + 1}, device_id_type=MESH)

    even = tm % 2 == 0

    @pl.when((tm > 1) & even)
    def _():
        pl.semaphore_signal(barrier, inc=1, device_id={"tm": tm - 2}, device_id_type=MESH)

    load_own = pltpu.make_async_copy(control, own, load_sem.at[0])
    load_own.start()
    load_counts = pltpu.make_async_copy(counts_in, counts, load_sem.at[1])
    load_counts.start()
    load_modes = pltpu.make_async_copy(modes_in, modes, load_sem.at[2])
    load_modes.start()

    def load(o, j, i, sem):
        pltpu.make_async_copy(
            perturbations.at[:, :, j, i, o], pert.at[:, :, j, i, o], load_sem.at[sem]).start()

    def loaded(o, j, i, sem):
        drain(pert.at[:, :, j, i, o], load_sem.at[sem])

    every = slice(None)
    groups = []
    for d in range(1, inner):
        groups.append((0, every, inner_peer(d)))
        for e in range(1, outer + 1):
            load(0, outer_peer(e), inner_peer(d), 2 + len(groups))
    for e in range(1, outer):
        groups.append((1, outer_peer(e), every))
        for d in range(1, inner + 1):
            load(1, outer_peer(e), inner_peer(d), 2 + len(groups))
    n_first = len(groups)
    groups.append((0, every, ix))
    for e in range(1, outer + 1):
        load(0, outer_peer(e), ix, 2 + len(groups))
    groups.append((1, jy, every))
    for d in range(1, inner + 1):
        load(1, jy, inner_peer(d), 2 + len(groups))

    row = lax.broadcasted_iota(jnp.int32, (1, level_rows, LANES), 1)
    lane = lax.broadcasted_iota(jnp.int32, (1, level_rows, LANES), 2)
    lon, half = row % nx, row // nx
    first_lon, last_lon = lon == 0, lon == nx - 1
    first_lane, last_lane = lane == 0, lane == LANES - 1
    has_next, has_prev = half < halves - 1, half > 0
    back = level_rows - 1

    def after(v):
        return pltpu.roll(v, level_rows - nx, 1)

    def before(v):
        return after(v) if halves == 2 else pltpu.roll(v, nx, 1)

    def spread(left, right):
        east = pltpu.roll(jnp.where(first_lon, before(right), 0.0), back, 1)
        west = pltpu.roll(jnp.where(last_lon, after(left), 0.0), 1, 1)
        return diffusion * (east + west)

    def relax(left, v, right):
        ahead, behind = after(v), before(v)
        east = pltpu.roll(jnp.where(first_lon, before(right), v), back, 1)
        west = pltpu.roll(jnp.where(last_lon, after(left), v), 1, 1)
        up = pltpu.roll(jnp.where(first_lane, jnp.where(has_next, ahead, 0.0), v), LANES - 1, 2)
        down = pltpu.roll(jnp.where(last_lane, jnp.where(has_prev, behind, 0.0), v), 1, 2)
        return (1.0 - 4.0 * diffusion) * v + diffusion * ((east + west) + (up + down))

    fields = own.shape[0]

    load_own.wait()
    zero = jnp.zeros((1, level_rows, LANES), jnp.float32)

    c = own[...]
    if tiles == 1:
        for _ in range(SMOOTH):
            c = relax(c, c, c)
    elif tiles == 2:
        c, o = relax(zero, c, zero), spread(c, c)
        for _ in range(1, SMOOTH):
            c, o = relax(o, c, o), relax(c, o, c)
        away[0] = o
    else:
        c, left, right = relax(zero, c, zero), spread(zero, c), spread(c, zero)
        for _ in range(1, SMOOTH):
            c, left, right = relax(left, c, right), relax(zero, left, c), relax(c, right, zero)
        away[0] = right
        away[1] = left
    smooth[...] = c

    chain_peers = jnp.where(tm > 0, 1, 0) + jnp.where(tm < steps_tm - 1, 1, 0)
    chain_peers = chain_peers + jnp.where(even & (tm < steps_tm - 2), 1, 0)
    pl.semaphore_wait(barrier, expected + chain_peers)

    halos = []
    for n, d in enumerate(tile_offsets):
        copy = pltpu.make_async_remote_copy(
            src_ref=away.at[n], dst_ref=near.at[n], send_sem=halo_send.at[n], recv_sem=halo_recv.at[n],
            device_id={"tile": (tile + d) % tiles}, device_id_type=MESH)
        copy.start()
        halos.append(copy)

    load_counts.wait()
    load_modes.wait()
    count = jnp.zeros((1, level_rows, LANES), jnp.int32)
    for x in range(nx):
        count = jnp.where(lon == x, counts[x], count)
    for copy in halos:
        copy.wait_recv()
    total = smooth[...]
    for n in range(len(tile_offsets)):
        total = total + near[n]
    mode = lax.broadcasted_iota(jnp.int32, (fields, level_rows, LANES), 0) % modes_n
    smooth[...] = jnp.where(mode < count, total * norm, 0.0)

    pair = 2 * level_rows

    def sums(o, c, j, i, u):
        base = (((j * inner + i) * 2 + o) * CHUNKS + c) * part_levels + 2 * u
        sizes = []
        for t in range(slots):
            acc = [[None] * 2 for _ in range(modes_n)]
            for k in range(members):
                x = pert[k, t, j, i, o, c, pl.ds(pl.multiple_of(u * pair, pair), pair), :].astype(jnp.float32)
                for m in range(modes_n):
                    s = smooth[k * modes_n + m]
                    for v in range(2):
                        term = s * x[v * level_rows:(v + 1) * level_rows]
                        acc[m][v] = term if k == 0 else acc[m][v] + term
            for v in range(2):
                total = modes[0, base + v] * acc[0][v]
                for m in range(1, modes_n):
                    total = total + modes[m, base + v] * acc[m][v]
                place = pl.ds(pl.multiple_of(u * pair + v * level_rows, level_rows), level_rows)
                if t < slots - 1:
                    part[1 + t, o, c, j, i, place, :] = total
                if t == 0:
                    sizes.append(total)
                else:
                    sizes[v] = sizes[v] + total
                if t == slots - 1:
                    part[0, o, c, j, i, place, :] = sizes[v]

    pairs = rows // pair

    def sums_over(count, place):
        def body(n, carry):
            u, n = n % pairs, n // pairs
            sums(*place(n), u)
            return carry

        lax.fori_loop(0, count * pairs, body, 0)

    def remote(src, dst, send, recv, to):
        return pltpu.make_async_remote_copy(
            src_ref=src, dst_ref=dst, send_sem=send, recv_sem=recv, device_id=to, device_id_type=MESH)

    steps_in, steps_out = range(1, inner), range(1, outer)
    pieces = pieces_of(slots)
    spans = [(f, pl.ds(c, n), c, n) for f, c, n in pieces]
    totals = [g for g, (f, _, _) in enumerate(pieces) if f == 0]
    others = [g for g, (f, _, _) in enumerate(pieces) if f > 0]

    rs1, rs2 = [[], []], [[], []]
    for g, (f, span, _, _) in enumerate(spans):
        rs1[0].append([remote(part.at[f, 0, span, :, inner_peer(d)], first_a.at[d - 1, f, span],
                              rs_send.at[0, d - 1], rs_recv.at[0, g, d - 1], at(jy, inner_peer(d)))
                       for d in steps_in])
        rs1[1].append([remote(part.at[f, 1, span, outer_peer(e)], first_b.at[e - 1, f, span],
                              rs_send.at[1, e - 1], rs_recv.at[1, g, e - 1], at(outer_peer(e), ix))
                       for e in steps_out])
        rs2[0].append([remote(mid_a.at[e - 1, f, span], second_a.at[e - 1, f, span],
                              rs_send.at[2, e - 1], rs_recv.at[2, g, e - 1], at(outer_peer(e), ix))
                       for e in steps_out])
        rs2[1].append([remote(mid_b.at[d - 1, f, span], second_b.at[d - 1, f, span],
                              rs_send.at[3, d - 1], rs_recv.at[3, g, d - 1], at(jy, inner_peer(d)))
                       for d in steps_in])

    for n, group in enumerate(groups[:n_first]):
        loaded(*group, 3 + n)
    for g in totals:
        _, _, c, _ = spans[g]
        for d, copy in zip(steps_in, rs1[0][g]):
            sums_over(outer, lambda n: (0, c, outer_peer(n), inner_peer(d)))
            copy.start()
        for e, copy in zip(steps_out, rs1[1][g]):
            sums_over(inner, lambda n: (1, c, outer_peer(e), inner_peer(n)))
            copy.start()
    for g in others:
        for o in range(2):
            for copy in rs1[o][g]:
                copy.start()
    for n, group in enumerate(groups[n_first:], n_first):
        loaded(*group, 3 + n)
    sums_over(CHUNKS * outer, lambda n: (0, n // outer, n % outer, ix))
    sums_over(CHUNKS * inner, lambda n: (1, n // inner, jy, n % inner))

    def second(g):
        f, span, _, _ = spans[g]
        for copy in rs1[0][g]:
            copy.wait_recv()
        for e, copy in zip(steps_out, rs2[0][g]):
            total = part[f, 0, span, outer_peer(e), ix]
            for d in steps_in:
                total = total + first_a[d - 1, f, span, outer_peer(e)]
            mid_a[e - 1, f, span] = total
            copy.start()
        for copy in rs1[1][g]:
            copy.wait_recv()
        for d, copy in zip(steps_in, rs2[1][g]):
            total = part[f, 1, span, jy, inner_peer(d)]
            for e in steps_out:
                total = total + first_b[e - 1, f, span, inner_peer(d)]
            mid_b[d - 1, f, span] = total
            copy.start()

    def gathers(g, o):
        f, span, _, _ = spans[g]
        sends, relays = [], []

        def move(j, i, to, kind, n):
            ref = ext.at[1 + f, j, i, o, span]
            recv = hop_recv.at[o, g, n] if kind == o else end_recv.at[o, 0 if kind == 2 else 1, n]
            return remote(ref, ref, ag_send.at[kind, n], recv, to)

        for d in steps_in:
            sends.append((0, d, move(jy, ix, at(jy, inner_peer(d)), 0, d - 1)))
        for e in steps_out:
            sends.append((1, e, move(jy, ix, at(outer_peer(e), ix), 1, e - 1)))
        for d in steps_in:
            for e in steps_out:
                n = (d - 1) * (outer - 1) + e - 1
                if o == 0:
                    relays.append((d, move(jy, inner_peer(inner - d), at(outer_peer(e), ix), 2, n)))
                else:
                    relays.append((e, move(outer_peer(outer - e), ix, at(jy, inner_peer(d)), 2, n)))
        return sends, relays

    slot_gathers = [[gathers(g, o) for o in range(2)] for g in range(len(pieces))]

    def relay(g, o):
        sends, relays = slot_gathers[g][o]
        for kind, d, copy in sends:
            if kind == o:
                copy.wait_recv()
                for dd, forward in relays:
                    if dd == d:
                        forward.start()

    def own_total(g, o):
        f, span, _, _ = spans[g]
        total = part[f, o, span, jy, ix]
        for copy in rs2[o][g]:
            copy.wait_recv()
        if o == 0:
            for d in steps_in:
                total = total + first_a[d - 1, f, span, jy]
            for e in steps_out:
                total = total + second_a[e - 1, f, span]
        else:
            for e in steps_out:
                total = total + first_b[e - 1, f, span, ix]
            for d in steps_in:
                total = total + second_b[d - 1, f, span]
        ext[1 + f, jy, ix, o, span] = total

    def up(c, src, step):
        dst = ext.at[0, jy, ix, :, c]
        return remote(src, dst, z_send.at[step - 1], z_recv.at[0, c], {"tm": tm + step})

    def side(c):
        return remote(ext.at[1, jy, ix, :, c], extra.at[c], z_send.at[0], z_recv.at[1, c], {"tm": tm + 1})

    def send_up(c, src):
        for step in range(1, min(3, steps_tm)):
            @pl.when(tm < steps_tm - step)
            def _():
                up(c, src, step).start()

    def early(c):
        ref = ext.at[0, jy, ix, :, c]
        targets = [(0, d - 1, at(jy, inner_peer(d))) for d in steps_in]
        targets += [(1, e - 1, at(outer_peer(e), ix)) for e in steps_out]
        targets += [(2, (d - 1) * (outer - 1) + e - 1, at(outer_peer(e), inner_peer(d)))
                    for d in steps_in for e in steps_out]
        return [remote(ref, ref, early_send.at[kind, n], early_recv.at[kind, n], to) for kind, n, to in targets]

    def earlier(c):
        up(c, extra.at[c], 1).wait_recv()

        @pl.when(even)
        def _():
            side(c).wait_recv()
            total = ext[0, jy, ix, :, c] + extra[c]
            ext[0, jy, ix, :, c] = total
            passing[c] = total + ext[1, jy, ix, :, c]
            send_up(c, passing.at[c])

        for copy in early(c):
            copy.start()

    for g in totals:
        second(g)
    for g in others:
        second(g)
    for g in totals:
        _, _, c, _ = spans[g]
        for o in range(2):
            own_total(g, o)

        @pl.when(tm == 0)
        def _():
            send_up(c, ext.at[1, jy, ix, :, c])

        @pl.when((tm % 2 == 1) & (tm < steps_tm - 1))
        def _():
            side(c).start()

        for o in range(2):
            for _, _, copy in slot_gathers[g][o][0]:
                copy.start()
    for g in others:
        for o in range(2):
            own_total(g, o)
            for _, _, copy in slot_gathers[g][o][0]:
                copy.start()

    near_first = (tm == 1) | (tm == 2)

    for g in totals:
        @pl.when(near_first)
        def _():
            earlier(spans[g][2])

        for o in range(2):
            relay(g, o)
    for g in others:
        for o in range(2):
            relay(g, o)

    @pl.when(tm > 2)
    def _():
        for g in totals:
            earlier(spans[g][2])

    @pl.when(tm == 0)
    def _():
        ext[0] = jnp.zeros(ext.shape[1:], jnp.float32)

    kinds = [(0, inner - 1), (1, outer - 1), (2, (inner - 1) * (outer - 1))]
    half = ext.at[pl.ds(1, slots), jy, ix, 0]
    whole = ext.at[pl.ds(1, slots), jy, ix]
    for o in range(2):
        for kind, count in kinds:
            if kind != o:
                for n in range(count):
                    drain(half, end_recv.at[o, 0 if kind == 2 else 1, n])
    for kind, count in kinds:
        for n in range(count):
            drain(whole, ag_send.at[kind, n])

    @pl.when(tm > 0)
    def _():
        for sems in (early_recv, early_send):
            for kind, count in kinds:
                for n in range(count):
                    drain(ext.at[0, jy, ix], sems.at[kind, n])

    @pl.when(tm < steps_tm - 1)
    def _():
        drain(passing, z_send.at[0])

    @pl.when(even & (tm < steps_tm - 2))
    def _():
        drain(passing, z_send.at[1])

    for copy in halos:
        copy.wait_send()
    for d in steps_in:
        drain(first_a.at[d - 1], rs_send.at[0, d - 1])
        drain(second_b.at[d - 1], rs_send.at[3, d - 1])
    for e in steps_out:
        drain(first_b.at[e - 1], rs_send.at[1, e - 1])
        drain(second_a.at[e - 1], rs_send.at[2, e - 1])


def blend(slots, ext, index, weight, out, held, sems):
    windows, total_rows, _ = out.shape
    size = total_rows // PIECES
    local = [index[w] - lax.axis_index("tm") * slots for w in range(windows)]
    shares = [[jnp.where(local[w] > t, 1.0, jnp.where(local[w] == t, weight[w], 0.0))
               for t in range(slots)] for w in range(windows)]
    factors = [[share[-1]] + [share[t] - share[-1] for t in range(slots - 1)] for share in shares]
    copies = []
    for n in range(PIECES):
        span = pl.ds(n * size, size)
        for w in range(windows):
            total = ext[0, span]
            for t in range(slots):
                total = total + factors[w][t] * ext[1 + t, span]
            held[w, span] = total
        copy = pltpu.make_async_copy(held.at[:, span], out.at[:, span], sems.at[n])
        copy.start()
        copies.append(copy)
    for copy in copies:
        copy.wait()


def pieces_of(slots):
    n = max(CHUNKS // 2, 1)
    return [(0, c, 1) for c in range(CHUNKS)] + [(f, c, n) for f in range(1, slots) for c in range(0, CHUNKS, n)]


def rows_view(x, nx, gy):
    lead = x.shape[:-2]
    x = x.reshape(lead + (nx, gy // LANES, LANES))
    x = jnp.swapaxes(x, -3, -2)
    return x


def per_device(control, vertical_modes, mode_counts, perturbations, slot_index, blend_weight):
    members, slots, levels, nx, gy = perturbations.shape
    modes_n = control.shape[1]
    halves = gy // LANES
    level_rows = nx * halves
    tiles, n_mem, steps_tm = lax.axis_size("tile"), lax.axis_size("mem"), lax.axis_size("tm")
    inner = 2 if n_mem % 2 == 0 else 1
    outer = n_mem // inner
    parts = 2 * CHUNKS
    rows = levels // (n_mem * parts) * level_rows
    assert nx >= SMOOTH and level_rows == 8 and rows % 16 == 0
    norm = 1.0 / math.sqrt(members * n_mem - 1)
    fields = members * modes_n
    c = rows_view(control, nx, gy).reshape(fields, level_rows, LANES)
    q = rows_view(perturbations, nx, gy).reshape(members, slots, outer, inner, 2, CHUNKS, rows, LANES)
    dims = (members, slots, modes_n, nx, halves, outer, inner, rows, tiles, steps_tm, norm)
    f32 = jnp.float32
    n_in, n_out = max(inner - 1, 1), max(outer - 1, 1)
    n_gather = max(inner - 1, outer - 1, (inner - 1) * (outer - 1), 1)
    n_pieces = len(pieces_of(slots))
    sides = 2 if tiles > 2 else 1
    dma = pltpu.SemaphoreType.DMA
    ext = pl.pallas_call(
        functools.partial(kernel, dims),
        out_shape=pltpu.VMEM((slots + 1, outer, inner, 2, CHUNKS, rows, LANES), f32),
        in_specs=[
            pl.BlockSpec(memory_space=pltpu.HBM),
            pl.BlockSpec(memory_space=pltpu.HBM),
            pl.BlockSpec(memory_space=pltpu.HBM),
            pl.BlockSpec(memory_space=pltpu.HBM),
        ],
        out_specs=pl.BlockSpec(memory_space=pltpu.VMEM),
        scratch_shapes=[
            pltpu.VMEM((fields, level_rows, LANES), f32),
            pltpu.VMEM((sides, fields, level_rows, LANES), f32),
            pltpu.VMEM((sides, fields, level_rows, LANES), f32),
            pltpu.VMEM(q.shape, q.dtype),
            pltpu.VMEM((fields, level_rows, LANES), f32),
            pltpu.VMEM((slots, 2, CHUNKS, outer, inner, rows, LANES), f32),
            pltpu.VMEM((n_in, slots, CHUNKS, outer, rows, LANES), f32),
            pltpu.VMEM((n_out, slots, CHUNKS, inner, rows, LANES), f32),
            pltpu.VMEM((n_out, slots, CHUNKS, rows, LANES), f32),
            pltpu.VMEM((n_in, slots, CHUNKS, rows, LANES), f32),
            pltpu.VMEM((n_out, slots, CHUNKS, rows, LANES), f32),
            pltpu.VMEM((n_in, slots, CHUNKS, rows, LANES), f32),
            pltpu.VMEM((CHUNKS, 2, rows, LANES), f32),
            pltpu.VMEM((CHUNKS, 2, rows, LANES), f32),
            pltpu.SMEM((modes_n, levels), f32),
            pltpu.SMEM((nx,), jnp.int32),
            dma((n_in + n_out + 5,)),
            dma((sides,)),
            dma((sides,)),
            dma((4, max(n_in, n_out))),
            dma((4, n_pieces, max(n_in, n_out))),
            dma((2,)),
            dma((2, CHUNKS)),
            dma((3, n_gather)),
            dma((2, n_pieces, max(n_in, n_out))),
            dma((2, 2, n_gather)),
            dma((3, n_gather)),
            dma((3, n_gather)),
        ],
        compiler_params=pltpu.CompilerParams(
            collective_id=0, has_side_effects=True),
    )(c, q, vertical_modes.T, mode_counts)
    ext = ext.reshape(slots + 1, levels * level_rows, LANES)
    windows = slot_index.shape[0]
    out = pl.pallas_call(
        functools.partial(blend, slots),
        out_shape=jax.ShapeDtypeStruct((windows, levels * level_rows, LANES), f32),
        in_specs=[
            pl.BlockSpec(memory_space=pltpu.VMEM),
            pl.BlockSpec(memory_space=pltpu.SMEM),
            pl.BlockSpec(memory_space=pltpu.SMEM),
        ],
        out_specs=pl.BlockSpec(memory_space=pltpu.HBM),
        scratch_shapes=[pltpu.VMEM((windows, levels * level_rows, LANES), f32), dma((PIECES,))],
        compiler_params=pltpu.CompilerParams(vmem_limit_bytes=8 << 20),
    )(ext, slot_index, blend_weight)
    out = out.reshape(windows, levels, halves, nx, LANES)
    return jnp.swapaxes(out, 2, 3).reshape(windows, levels, nx, gy)


def solution(mesh):
    placed = (
        P("mem", None, "tile", None),
        P(),
        P("tile"),
        P("mem", "tm", None, "tile", None),
        P("tm"),
        P("tm"),
    )
    return jax.shard_map(
        per_device,
        mesh=mesh,
        in_specs=placed,
        out_specs=P("tm", None, "tile", None),
        check_vma=False,
    )
```

```python
import functools
import math

import jax
import jax.numpy as jnp
from jax import lax
from jax.experimental import pallas as pl
from jax.experimental.pallas import tpu as pltpu
from jax.sharding import PartitionSpec as P

SMOOTH = 4
CHUNKS = 4
LANES = 128
MESH = pl.DeviceIdType.MESH

diffusion = 0.24


def drain(ref, sem):
    pltpu.make_async_copy(ref, ref, sem).wait()


def kernel(dims, control, perturbations, modes_in, counts_in, index_in, weight_in, out, ext, own, near, away, pert,
           smooth, part, arrived, extra, passing, modes, counts, index, weight,
           load_sem, pert_sem, halo_send, halo_recv, rs_send, rs_recv, z_send, z_recv, ag_send, hop_recv, end_recv,
           early_send, early_recv):
    members, slots, modes_n, nx, halves, outer, inner, rows, tiles, steps_tm, norm = dims
    tm = lax.axis_index("tm")
    mem = lax.axis_index("mem")
    tile = lax.axis_index("tile")
    jy, ix = mem // inner, mem % inner
    level_rows = nx * halves
    part_levels = rows // level_rows

    def inner_peer(d):
        return (ix + d) % inner

    def outer_peer(d):
        return (jy + d) % outer

    def at(j, i):
        return {"mem": j * inner + i}

    barrier = pltpu.get_barrier_semaphore()
    tile_offsets = sorted({1 % tiles, (tiles - 1) % tiles} - {0})
    expected = len(tile_offsets) + inner * outer - 1
    for e in range(1, outer):
        for d in range(1, inner):
            pl.semaphore_signal(barrier, inc=1, device_id=at(outer_peer(e), inner_peer(d)), device_id_type=MESH)
    for d in tile_offsets:
        pl.semaphore_signal(barrier, inc=1, device_id={"tile": (tile + d) % tiles}, device_id_type=MESH)
    for d in range(1, inner):
        pl.semaphore_signal(barrier, inc=1, device_id=at(jy, inner_peer(d)), device_id_type=MESH)
    for e in range(1, outer):
        pl.semaphore_signal(barrier, inc=1, device_id=at(outer_peer(e), ix), device_id_type=MESH)

    @pl.when(tm > 0)
    def _():
        pl.semaphore_signal(barrier, inc=1, device_id={"tm": tm - 1}, device_id_type=MESH)

    @pl.when(tm < steps_tm - 1)
    def _():
        pl.semaphore_signal(barrier, inc=1, device_id={"tm": tm + 1}, device_id_type=MESH)

    even = tm % 2 == 0

    @pl.when((tm > 1) & even)
    def _():
        pl.semaphore_signal(barrier, inc=1, device_id={"tm": tm - 2}, device_id_type=MESH)

    load_own = pltpu.make_async_copy(control, own, load_sem.at[0])
    load_own.start()
    load_counts = pltpu.make_async_copy(counts_in, counts, load_sem.at[1])
    load_counts.start()
    load_modes = pltpu.make_async_copy(modes_in, modes, load_sem.at[2])
    load_modes.start()
    load_index = pltpu.make_async_copy(index_in, index, load_sem.at[3])
    load_index.start()
    load_weight = pltpu.make_async_copy(weight_in, weight, load_sem.at[4])
    load_weight.start()

    offsets = sorted(((e, d) for e in range(outer) for d in range(inner)), key=lambda ed: -(ed[0] > 0) - (ed[1] > 0))
    blocks = [(outer_peer(e), inner_peer(d)) for e, d in offsets]
    pert_loads = []
    for n, (j, i) in enumerate(blocks):
        copy = pltpu.make_async_copy(perturbations.at[:, :, j, i], pert.at[:, :, j, i], pert_sem.at[n])
        copy.start()
        pert_loads.append(copy)

    row = lax.broadcasted_iota(jnp.int32, (1, level_rows, LANES), 1)
    lane = lax.broadcasted_iota(jnp.int32, (1, level_rows, LANES), 2)
    lon, half = row % nx, row // nx
    first_lon, last_lon = lon == 0, lon == nx - 1
    first_lane, last_lane = lane == 0, lane == LANES - 1
    has_next, has_prev = half < halves - 1, half > 0
    back = level_rows - 1

    def after(v):
        return pltpu.roll(v, level_rows - nx, 1)

    def before(v):
        return after(v) if halves == 2 else pltpu.roll(v, nx, 1)

    def spread(left, right):
        east = pltpu.roll(jnp.where(first_lon, before(right), 0.0), back, 1)
        west = pltpu.roll(jnp.where(last_lon, after(left), 0.0), 1, 1)
        return diffusion * (east + west)

    def relax(left, v, right):
        ahead, behind = after(v), before(v)
        east = pltpu.roll(jnp.where(first_lon, before(right), v), back, 1)
        west = pltpu.roll(jnp.where(last_lon, after(left), v), 1, 1)
        up = pltpu.roll(jnp.where(first_lane, jnp.where(has_next, ahead, 0.0), v), LANES - 1, 2)
        down = pltpu.roll(jnp.where(last_lane, jnp.where(has_prev, behind, 0.0), v), 1, 2)
        return (1.0 - 4.0 * diffusion) * v + diffusion * ((east + west) + (up + down))

    fields = own.shape[0]

    load_own.wait()
    zero = jnp.zeros((1, level_rows, LANES), jnp.float32)

    c = own[...]
    if tiles == 1:
        for _ in range(SMOOTH):
            c = relax(c, c, c)
    elif tiles == 2:
        c, o = relax(zero, c, zero), spread(c, c)
        for _ in range(1, SMOOTH):
            c, o = relax(o, c, o), relax(c, o, c)
        away[0] = o
    else:
        c, left, right = relax(zero, c, zero), spread(zero, c), spread(c, zero)
        for _ in range(1, SMOOTH):
            c, left, right = relax(left, c, right), relax(zero, left, c), relax(c, right, zero)
        away[0] = right
        away[1] = left
    smooth[...] = c

    chain_peers = jnp.where(tm > 0, 1, 0) + jnp.where(tm < steps_tm - 1, 1, 0)
    chain_peers = chain_peers + jnp.where(even & (tm < steps_tm - 2), 1, 0)
    pl.semaphore_wait(barrier, expected + chain_peers)

    halos = []
    for n, d in enumerate(tile_offsets):
        copy = pltpu.make_async_remote_copy(
            src_ref=away.at[n], dst_ref=near.at[n], send_sem=halo_send.at[n], recv_sem=halo_recv.at[n],
            device_id={"tile": (tile + d) % tiles}, device_id_type=MESH)
        copy.start()
        halos.append(copy)

    load_counts.wait()
    load_modes.wait()
    load_index.wait()
    load_weight.wait()
    count = jnp.zeros((1, level_rows, LANES), jnp.int32)
    for x in range(nx):
        count = jnp.where(lon == x, counts[x], count)
    for copy in halos:
        copy.wait_recv()
    total = smooth[...]
    for n in range(len(tile_offsets)):
        total = total + near[n]
    mode = lax.broadcasted_iota(jnp.int32, (fields, level_rows, LANES), 0) % modes_n
    smooth[...] = jnp.where(mode < count, total * norm, 0.0)

    pair = 2 * level_rows

    def sums(o, c, j, i, u):
        base = (((j * inner + i) * 2 + o) * CHUNKS + c) * part_levels + 2 * u
        sizes = []
        for t in range(slots):
            acc = [[None] * 2 for _ in range(modes_n)]
            for k in range(members):
                x = pert[k, t, j, i, o, c, pl.ds(pl.multiple_of(u * pair, pair), pair), :].astype(jnp.float32)
                for m in range(modes_n):
                    s = smooth[k * modes_n + m]
                    for v in range(2):
                        term = s * x[v * level_rows:(v + 1) * level_rows]
                        acc[m][v] = term if k == 0 else acc[m][v] + term
            for v in range(2):
                total = modes[0, base + v] * acc[0][v]
                for m in range(1, modes_n):
                    total = total + modes[m, base + v] * acc[m][v]
                place = pl.ds(pl.multiple_of(u * pair + v * level_rows, level_rows), level_rows)
                if t < slots - 1:
                    part[1 + t, o, c, j, i, place, :] = total
                if t == 0:
                    sizes.append(total)
                else:
                    sizes[v] = sizes[v] + total
                if t == slots - 1:
                    part[0, o, c, j, i, place, :] = sizes[v]

    pairs = rows // pair

    def sums_over(count, place):
        def body(n, carry):
            u, n = n % pairs, n // pairs
            sums(*place(n), u)
            return carry

        lax.fori_loop(0, count * pairs, body, 0)

    def remote(src, dst, send, recv, to):
        return pltpu.make_async_remote_copy(
            src_ref=src, dst_ref=dst, send_sem=send, recv_sem=recv, device_id=to, device_id_type=MESH)

    steps_in, steps_out = range(1, inner), range(1, outer)
    pieces = pieces_of(slots)
    spans = [(f, pl.ds(c, n), c, n) for f, c, n in pieces]
    totals = [g for g, (f, _, _) in enumerate(pieces) if f == 0]
    others = [g for g, (f, _, _) in enumerate(pieces) if f > 0]

    blocks = blocks[:-1]
    scatter = [[remote(part.at[f, :, span, j, i], arrived.at[k, f, :, span], rs_send, rs_recv.at[g], at(j, i))
                for k, (j, i) in enumerate(blocks)] for g, (f, span, _, _) in enumerate(spans)]

    for g in totals:
        c = spans[g][2]
        for k, (j, i) in enumerate(blocks):
            if g == 0:
                pert_loads[k].wait()
            sums_over(2, lambda n: (n, c, j, i))
            scatter[g][k].start()
    for g in others:
        for copy in scatter[g]:
            copy.start()
    pert_loads[-1].wait()
    sums_over(2 * CHUNKS, lambda n: (n % 2, n // 2, jy, ix))

    def gathers(g, o):
        f, span, _, _ = spans[g]
        sends, relays = [], []

        def move(j, i, to, kind, n):
            ref = ext.at[1 + f, j, i, o, span]
            return remote(ref, ref, ag_send, hop_recv.at[o, g, n] if kind == o else end_recv.at[o], to)

        for d in steps_in:
            sends.append((0, d, move(jy, ix, at(jy, inner_peer(d)), 0, d - 1)))
        for e in steps_out:
            sends.append((1, e, move(jy, ix, at(outer_peer(e), ix), 1, e - 1)))
        for d in steps_in:
            for e in steps_out:
                n = 0
                if o == 0:
                    relays.append((d, move(jy, inner_peer(inner - d), at(outer_peer(e), ix), 2, n)))
                else:
                    relays.append((e, move(outer_peer(outer - e), ix, at(jy, inner_peer(d)), 2, n)))
        return sends, relays

    slot_gathers = [[gathers(g, o) for o in range(2)] for g in range(len(pieces))]

    def across(g, o):
        f, span, _, _ = spans[g]
        ref = ext.at[1 + f, jy, ix, o, span]
        for d in steps_in:
            for e in steps_out:
                remote(ref, ref, ag_send, end_recv.at[o], at(outer_peer(e), inner_peer(d))).start()

    def share(g):
        for o in range(2):
            for _, _, copy in slot_gathers[g][o][0]:
                copy.start()
            if g in others:
                @pl.when(tm == 0)
                def _():
                    across(g, o)

    def relay(g):
        for o in range(2):
            sends, relays = slot_gathers[g][o]
            for kind, d, copy in sends:
                if kind == o:
                    copy.wait_recv()
                    for dd, forward in relays:
                        if dd == d:
                            if g in others:
                                @pl.when(tm > 0)
                                def _():
                                    forward.start()
                            else:
                                forward.start()

    def own_total(g):
        f, span, _, _ = spans[g]
        total = part[f, :, span, jy, ix]
        if blocks:
            drain(arrived.at[:, f, :, span], rs_recv.at[g])
        for k in range(len(blocks)):
            total = total + arrived[k, f, :, span]
        ext[1 + f, jy, ix, :, span] = total

    def up(c, src, step):
        dst = ext.at[0, jy, ix, :, c]
        return remote(src, dst, z_send.at[step - 1], z_recv.at[0, c], {"tm": tm + step})

    def side(c):
        return remote(ext.at[1, jy, ix, :, c], extra.at[c], z_send.at[0], z_recv.at[1, c], {"tm": tm + 1})

    def send_up(c, src, steps=(2, 1)):
        for step in (k for k in steps if k < steps_tm):
            @pl.when(tm < steps_tm - step)
            def _():
                up(c, src, step).start()

    def early(c):
        ref = ext.at[0, jy, ix, :, c]
        return [remote(ref, ref, early_send, early_recv, at(j, i)) for j, i in blocks]

    def earlier(c):
        up(c, extra.at[c], 1).wait_recv()

        @pl.when(even)
        def _():
            side(c).wait_recv()
            total = ext[0, jy, ix, :, c] + extra[c]
            ext[0, jy, ix, :, c] = total
            passing[c] = total + ext[1, jy, ix, :, c]
            send_up(c, passing.at[c])

    def share_earlier(c):
        for copy in early(c):
            copy.start()

    for g in totals:
        c = spans[g][2]
        own_total(g)

        @pl.when(tm == 0)
        def _():
            send_up(c, ext.at[1, jy, ix, :, c])

        @pl.when((tm % 2 == 1) & (tm < steps_tm - 1))
        def _():
            side(c).start()

        share(g)
    chunks = list(range(CHUNKS))
    for n, g in enumerate(others):
        own_total(g)
        share(g)
        last = n == len(others) - 1

        @pl.when((tm > 0) & even)
        def _():
            for c in chunks[:-1] if n == 0 and not last else chunks[-1:] if last and n > 0 else chunks if last else []:
                earlier(c)

    @pl.when((tm > 0) & even)
    def _():
        for c in chunks:
            share_earlier(c)

    for g in totals:
        relay(g)

    @pl.when(tm == 1)
    def _():
        for c in chunks:
            earlier(c)
            share_earlier(c)

    for n, g in enumerate(others):
        @pl.when((tm > 1) & (tm % 2 == 1))
        def _():
            for c in chunks[n * CHUNKS // len(others):(n + 1) * CHUNKS // len(others)]:
                earlier(c)
                share_earlier(c)

        relay(g)

    if outer > 1:
        drain(ext.at[pl.ds(1, slots), pl.ds(0, outer - 1), :, 0], end_recv.at[0])
    if inner > 1:
        drain(ext.at[pl.ds(1, slots), :, pl.ds(0, inner - 1), 1], end_recv.at[1])

    windows = out.shape[0]
    local = [index[w] - tm * slots for w in range(windows)]
    shares = [[jnp.where(local[w] > t, 1.0, jnp.where(local[w] == t, weight[w], 0.0))
               for t in range(slots)] for w in range(windows)]
    factors = [[share[-1]] + [share[t] - share[-1] for t in range(slots - 1)] for share in shares]

    def each_block(body):
        def step(n, carry):
            body(n // (inner * 2), n // 2 % inner, n % 2)
            return carry

        lax.fori_loop(0, outer * inner * 2, step, 0)

    @each_block
    def _(j, i, o):
        for w in range(windows):
            total = factors[w][0] * ext[1, j, i, o]
            for t in range(1, slots):
                total = total + factors[w][t] * ext[1 + t, j, i, o]
            out[w, j, i, o] = total

    @pl.when(tm < steps_tm - 1)
    def _():
        drain(passing, z_send.at[0])

    @pl.when(even & (tm < steps_tm - 2))
    def _():
        drain(passing, z_send.at[1])

    for copy in halos:
        copy.wait_send()
    if blocks:
        drain(arrived, rs_send)
        drain(arrived, ag_send)

    @pl.when(tm > 0)
    def _():
        if blocks:
            drain(arrived.at[:, 0], early_send)
            drain(arrived.at[:, 0], early_recv)

        @each_block
        def _(j, i, o):
            total = ext[0, j, i, o]
            for w in range(windows):
                out[w, j, i, o] = out[w, j, i, o] + total


def store(held, out, sem):
    copy = pltpu.make_async_copy(held, out, sem)
    copy.start()
    copy.wait()


def pieces_of(slots):
    n = max(CHUNKS // 2, 1)
    return [(0, c, 1) for c in range(CHUNKS)] + [(f, c, n) for f in range(1, slots) for c in range(0, CHUNKS, n)]


def rows_view(x, nx, gy):
    lead = x.shape[:-2]
    x = x.reshape(lead + (nx, gy // LANES, LANES))
    x = jnp.swapaxes(x, -3, -2)
    return x


def per_device(control, vertical_modes, mode_counts, perturbations, slot_index, blend_weight):
    members, slots, levels, nx, gy = perturbations.shape
    modes_n = control.shape[1]
    halves = gy // LANES
    level_rows = nx * halves
    tiles, n_mem, steps_tm = lax.axis_size("tile"), lax.axis_size("mem"), lax.axis_size("tm")
    inner = 2 if n_mem % 2 == 0 else 1
    outer = n_mem // inner
    parts = 2 * CHUNKS
    rows = levels // (n_mem * parts) * level_rows
    assert nx >= SMOOTH and level_rows == 8 and rows % 16 == 0
    norm = 1.0 / math.sqrt(members * n_mem - 1)
    fields = members * modes_n
    c = rows_view(control, nx, gy).reshape(fields, level_rows, LANES)
    q = rows_view(perturbations, nx, gy).reshape(members, slots, outer, inner, 2, CHUNKS, rows, LANES)
    dims = (members, slots, modes_n, nx, halves, outer, inner, rows, tiles, steps_tm, norm)
    f32 = jnp.float32
    n_in, n_out = max(inner - 1, 1), max(outer - 1, 1)
    n_pieces = len(pieces_of(slots))
    sides = 2 if tiles > 2 else 1
    dma = pltpu.SemaphoreType.DMA
    windows = slot_index.shape[0]
    held = pl.pallas_call(
        functools.partial(kernel, dims),
        out_shape=pltpu.VMEM((windows, outer, inner, 2, CHUNKS, rows, LANES), f32),
        in_specs=[
            pl.BlockSpec(memory_space=pltpu.HBM),
            pl.BlockSpec(memory_space=pltpu.HBM),
            pl.BlockSpec(memory_space=pltpu.HBM),
            pl.BlockSpec(memory_space=pltpu.HBM),
            pl.BlockSpec(memory_space=pltpu.HBM),
            pl.BlockSpec(memory_space=pltpu.HBM),
        ],
        out_specs=pl.BlockSpec(memory_space=pltpu.VMEM),
        scratch_shapes=[
            pltpu.VMEM((slots + 1, outer, inner, 2, CHUNKS, rows, LANES), f32),
            pltpu.VMEM((fields, level_rows, LANES), f32),
            pltpu.VMEM((sides, fields, level_rows, LANES), f32),
            pltpu.VMEM((sides, fields, level_rows, LANES), f32),
            pltpu.VMEM(q.shape, q.dtype),
            pltpu.VMEM((fields, level_rows, LANES), f32),
            pltpu.VMEM((slots, 2, CHUNKS, outer, inner, rows, LANES), f32),
            pltpu.VMEM((max(n_mem - 1, 1), slots, 2, CHUNKS, rows, LANES), f32),
            pltpu.VMEM((CHUNKS, 2, rows, LANES), f32),
            pltpu.VMEM((CHUNKS, 2, rows, LANES), f32),
            pltpu.SMEM((modes_n, levels), f32),
            pltpu.SMEM((nx,), jnp.int32),
            pltpu.SMEM((windows,), jnp.int32),
            pltpu.SMEM((windows,), f32),
            dma((5,)),
            dma((n_mem,)),
            dma((sides,)),
            dma((sides,)),
            dma,
            dma((n_pieces,)),
            dma((2,)),
            dma((2, CHUNKS)),
            dma,
            dma((2, n_pieces, max(n_in, n_out))),
            dma((2,)),
            dma,
            dma,
        ],
        compiler_params=pltpu.CompilerParams(
            collective_id=0, has_side_effects=True),
    )(c, q, vertical_modes.T, mode_counts, slot_index, blend_weight)
    held = held.reshape(windows, levels * level_rows, LANES)
    out = pl.pallas_call(
        store,
        out_shape=jax.ShapeDtypeStruct((windows, levels * level_rows, LANES), f32),
        in_specs=[pl.BlockSpec(memory_space=pltpu.VMEM)],
        out_specs=pl.BlockSpec(memory_space=pltpu.HBM),
        scratch_shapes=[dma],
        compiler_params=pltpu.CompilerParams(vmem_limit_bytes=8 << 20),
    )(held)
    out = out.reshape(windows, levels, halves, nx, LANES)
    return jnp.swapaxes(out, 2, 3).reshape(windows, levels, nx, gy)


def solution(mesh):
    placed = (
        P("mem", None, "tile", None),
        P(),
        P("tile"),
        P("mem", "tm", None, "tile", None),
        P("tm"),
        P("tm"),
    )
    return jax.shard_map(
        per_device,
        mesh=mesh,
        in_specs=placed,
        out_specs=P("tm", None, "tile", None),
        check_vma=False,
    )
```

```python
import functools
import math

import jax
import jax.numpy as jnp
import numpy as np
from jax import lax
from jax.experimental import pallas as pl
from jax.experimental.pallas import tpu as pltpu
from jax.sharding import PartitionSpec as P

SMOOTH = 4
CHUNKS = 4
STORES = 8
LANES = 128
MESH = pl.DeviceIdType.MESH

diffusion = 0.24


def drain(ref, sem):
    pltpu.make_async_copy(ref, ref, sem).wait()


def kernel(dims, control, perturbations, modes_in, counts_in, index_in, weight_in, out, ext, own, near, away, pert,
           smooth, part, arrived, extra, passing, modes, counts, index, weight,
           load_sem, pert_sem, halo_send, halo_recv, rs_send, rs_recv, z_send, z_recv, ag_send, hop_recv, end_recv,
           early_send, early_recv, ready):
    members, slots, modes_n, nx, halves, outer, inner, rows, tiles, steps_tm, norm = dims
    tm = lax.axis_index("tm")
    mem = lax.axis_index("mem")
    tile = lax.axis_index("tile")
    jy, ix = mem // inner, mem % inner
    level_rows = nx * halves
    part_levels = rows // level_rows

    def inner_peer(d):
        return (ix + d) % inner

    def outer_peer(d):
        return (jy + d) % outer

    def at(j, i):
        return {"mem": j * inner + i}

    barrier = pltpu.get_barrier_semaphore()
    tile_offsets = sorted({1 % tiles, (tiles - 1) % tiles} - {0})
    expected = len(tile_offsets) + inner - 1 + outer - 1
    for d in tile_offsets:
        pl.semaphore_signal(barrier, inc=1, device_id={"tile": (tile + d) % tiles}, device_id_type=MESH)
    for d in range(1, inner):
        pl.semaphore_signal(barrier, inc=1, device_id=at(jy, inner_peer(d)), device_id_type=MESH)
    for e in range(1, outer):
        pl.semaphore_signal(barrier, inc=1, device_id=at(outer_peer(e), ix), device_id_type=MESH)

    @pl.when(tm > 0)
    def _():
        pl.semaphore_signal(barrier, inc=1, device_id={"tm": tm - 1}, device_id_type=MESH)

    @pl.when(tm < steps_tm - 1)
    def _():
        pl.semaphore_signal(barrier, inc=1, device_id={"tm": tm + 1}, device_id_type=MESH)

    even = tm % 2 == 0

    @pl.when((tm > 1) & even)
    def _():
        pl.semaphore_signal(barrier, inc=1, device_id={"tm": tm - 2}, device_id_type=MESH)

    load_own = pltpu.make_async_copy(control, own, load_sem.at[0])
    load_own.start()
    load_counts = pltpu.make_async_copy(counts_in, counts, load_sem.at[1])
    load_counts.start()
    load_modes = pltpu.make_async_copy(modes_in, modes, load_sem.at[2])
    load_modes.start()
    load_index = pltpu.make_async_copy(index_in, index, load_sem.at[3])
    load_index.start()
    load_weight = pltpu.make_async_copy(weight_in, weight, load_sem.at[4])
    load_weight.start()

    offsets = sorted(((e, d) for e in range(outer) for d in range(inner)), key=lambda ed: ((ed[0] > 0) + (ed[1] > 0) - 1) % 3)
    blocks = [(outer_peer(e), inner_peer(d)) for e, d in offsets]
    pert_loads = []
    for n, (j, i) in enumerate(blocks):
        copy = pltpu.make_async_copy(perturbations.at[:, :, j, i], pert.at[:, :, j, i], pert_sem.at[n])
        copy.start()
        pert_loads.append(copy)

    row = lax.broadcasted_iota(jnp.int32, (1, level_rows, LANES), 1)
    lane = lax.broadcasted_iota(jnp.int32, (1, level_rows, LANES), 2)
    lon, half = row % nx, row // nx
    first_lon, last_lon = lon == 0, lon == nx - 1
    first_lane, last_lane = lane == 0, lane == LANES - 1
    has_next, has_prev = half < halves - 1, half > 0
    back = level_rows - 1

    def after(v):
        return pltpu.roll(v, level_rows - nx, 1)

    def before(v):
        return after(v) if halves == 2 else pltpu.roll(v, nx, 1)

    def spread(left, right):
        east = pltpu.roll(jnp.where(first_lon, before(right), 0.0), back, 1)
        west = pltpu.roll(jnp.where(last_lon, after(left), 0.0), 1, 1)
        return diffusion * (east + west)

    def relax(left, v, right):
        ahead, behind = after(v), before(v)
        east = pltpu.roll(jnp.where(first_lon, before(right), v), back, 1)
        west = pltpu.roll(jnp.where(last_lon, after(left), v), 1, 1)
        up = pltpu.roll(jnp.where(first_lane, jnp.where(has_next, ahead, 0.0), v), LANES - 1, 2)
        down = pltpu.roll(jnp.where(last_lane, jnp.where(has_prev, behind, 0.0), v), 1, 2)
        return (1.0 - 4.0 * diffusion) * v + diffusion * ((east + west) + (up + down))

    def diffuse_pair(v):
        at_step = binomial_rings(2 * nx)

        crossing = (first_lane & has_next) | (last_lane & has_prev)
        powers = [v]
        for _ in range(SMOOTH):
            v = powers[-1]
            edge = jnp.where(crossing, pltpu.roll(v, nx, 1), 0.0)
            above, below = jnp.where(first_lane, edge, v), jnp.where(last_lane, edge, v)
            powers.append(pltpu.roll(above, LANES - 1, 2) + pltpu.roll(below, 1, 2))

        def mix(distance):
            total = None
            for k, term in enumerate(powers):
                if at_step[k][distance] != 0.0:
                    part = at_step[k][distance] * term
                    total = part if total is None else total + part
            return total

        here = [mix(m) for m in range(nx + 1)]
        there = [pltpu.roll(here[m], nx, 1) for m in range(1, nx)]
        centre, other = here[0], here[nx]
        for m in range(1, nx):
            inside = lon + m < nx
            centre = centre + pltpu.roll(jnp.where(inside, here[m], there[nx - m - 1]), m, 1)
            other = other + pltpu.roll(jnp.where(inside, here[nx - m], there[m - 1]), m, 1)
        return centre, other

    fields = own.shape[0]

    load_own.wait()
    zero = jnp.zeros((1, level_rows, LANES), jnp.float32)

    c = own[...]
    if tiles == 1:
        for _ in range(SMOOTH):
            c = relax(c, c, c)
    elif tiles == 2 and halves == 2:
        batch = fields // 2 if fields % 2 == 0 else fields
        parts = []
        for n in range(0, fields, batch):
            centre, away[0, n:n + batch] = diffuse_pair(c[n:n + batch])
            parts.append(centre)
        c = jnp.concatenate(parts, axis=0)
    elif tiles == 2:
        c, o = relax(zero, c, zero), spread(c, c)
        for _ in range(1, SMOOTH):
            c, o = relax(o, c, o), relax(c, o, c)
        away[0] = o
    else:
        c, left, right = relax(zero, c, zero), spread(zero, c), spread(c, zero)
        for _ in range(1, SMOOTH):
            c, left, right = relax(left, c, right), relax(zero, left, c), relax(c, right, zero)
        away[0] = right
        away[1] = left
    smooth[...] = c

    chain_peers = jnp.where(tm > 0, 1, 0) + jnp.where(tm < steps_tm - 1, 1, 0)
    chain_peers = chain_peers + jnp.where(even & (tm < steps_tm - 2), 1, 0)
    pl.semaphore_wait(barrier, expected + chain_peers)

    for d in range(1, inner):
        pl.semaphore_signal(ready, inc=1, device_id=at(jy, inner_peer(d)), device_id_type=MESH)

    halos = []
    for n, d in enumerate(tile_offsets):
        copy = pltpu.make_async_remote_copy(
            src_ref=away.at[n], dst_ref=near.at[n], send_sem=halo_send.at[n], recv_sem=halo_recv.at[n],
            device_id={"tile": (tile + d) % tiles}, device_id_type=MESH)
        copy.start()
        halos.append(copy)

    load_counts.wait()
    load_modes.wait()
    load_index.wait()
    load_weight.wait()
    count = jnp.zeros((1, level_rows, LANES), jnp.int32)
    for x in range(nx):
        count = jnp.where(lon == x, counts[x], count)
    for copy in halos:
        copy.wait_recv()
    total = smooth[...]
    for n in range(len(tile_offsets)):
        total = total + near[n]
    mode = lax.broadcasted_iota(jnp.int32, (fields, level_rows, LANES), 0) % modes_n
    smooth[...] = jnp.where(mode < count, total * norm, 0.0)

    pair = 2 * level_rows

    def sums(o, c, j, i, u):
        base = (((j * inner + i) * 2 + o) * CHUNKS + c) * part_levels + 2 * u
        sizes = []
        for t in range(slots):
            acc = [[None] * 2 for _ in range(modes_n)]
            for k in range(members):
                x = pert[k, t, j, i, o, c, pl.ds(pl.multiple_of(u * pair, pair), pair), :].astype(jnp.float32)
                for m in range(modes_n):
                    s = smooth[k * modes_n + m]
                    for v in range(2):
                        term = s * x[v * level_rows:(v + 1) * level_rows]
                        acc[m][v] = term if k == 0 else acc[m][v] + term
            for v in range(2):
                total = modes[0, base + v] * acc[0][v]
                for m in range(1, modes_n):
                    total = total + modes[m, base + v] * acc[m][v]
                place = pl.ds(pl.multiple_of(u * pair + v * level_rows, level_rows), level_rows)
                if t < slots - 1:
                    part[1 + t, o, c, j, i, place, :] = total
                if t == 0:
                    sizes.append(total)
                else:
                    sizes[v] = sizes[v] + total
                if t == slots - 1:
                    part[0, o, c, j, i, place, :] = sizes[v]

    pairs = rows // pair

    def sums_over(count, place):
        def body(n, carry):
            u, n = n % pairs, n // pairs
            sums(*place(n), u)
            return carry

        lax.fori_loop(0, count * pairs, body, 0)

    def remote(src, dst, send, recv, to):
        return pltpu.make_async_remote_copy(
            src_ref=src, dst_ref=dst, send_sem=send, recv_sem=recv, device_id=to, device_id_type=MESH)

    steps_in, steps_out = range(1, inner), range(1, outer)
    pieces = pieces_of(slots)
    spans = [(f, pl.ds(c, n), c, n) for f, c, n in pieces]
    totals = [g for g, (f, _, _) in enumerate(pieces) if f == 0]
    others = [g for g, (f, _, _) in enumerate(pieces) if f > 0]

    blocks = blocks[:-1]
    scatter = [[remote(part.at[f, :, span, j, i], arrived.at[k, f, :, span], rs_send, rs_recv.at[g], at(j, i))
                for k, (j, i) in enumerate(blocks)] for g, (f, span, _, _) in enumerate(spans)]

    near_ks = [k for k, (e, d) in enumerate(offsets[:-1]) if e == 0 or d == 0]
    far_ks = [k for k in range(len(blocks)) if k not in near_ks]
    for ks in (near_ks, far_ks):
        for g in totals:
            c = spans[g][2]
            for k in ks:
                j, i = blocks[k]
                if g == 0:
                    pert_loads[k].wait()
                sums_over(2, lambda n: (n, c, j, i))
                if g == 0 and far_ks and k == far_ks[0]:
                    pl.semaphore_wait(ready, inner - 1)
                scatter[g][k].start()
    for g in others:
        for copy in scatter[g]:
            copy.start()
    pert_loads[-1].wait()
    sums_over(2 * CHUNKS, lambda n: (n % 2, n // 2, jy, ix))

    def last_kind(f, kind):
        return 0 if f == 0 else 1 + (kind == 2)

    def gathers(g, o):
        f, span, _, _ = spans[g]
        sends, relays = [], []

        def move(j, i, to, kind, n):
            ref = ext.at[1 + f, j, i, o, span]
            return remote(ref, ref, ag_send, hop_recv.at[o, g, n] if kind == o else end_recv.at[o, last_kind(f, kind)], to)

        for d in steps_in:
            sends.append((0, d, move(jy, ix, at(jy, inner_peer(d)), 0, d - 1)))
        for e in steps_out:
            sends.append((1, e, move(jy, ix, at(outer_peer(e), ix), 1, e - 1)))
        for d in steps_in:
            for e in steps_out:
                if o == 0:
                    relays.append((d, move(jy, inner_peer(inner - d), at(outer_peer(e), ix), 2, n)))
                else:
                    relays.append((e, move(outer_peer(outer - e), ix, at(jy, inner_peer(d)), 2, n)))
        return sends, relays

    slot_gathers = [[gathers(g, o) for o in range(2)] for g in range(len(pieces))]

    def across(g, o):
        f, span, _, _ = spans[g]
        ref = ext.at[1 + f, jy, ix, o, span]
        for d in steps_in:
            for e in steps_out:
                remote(ref, ref, ag_send, end_recv.at[o, last_kind(f, 2)], at(outer_peer(e), inner_peer(d))).start()

    def share(g):
        for o in range(2):
            for _, _, copy in slot_gathers[g][o][0]:
                copy.start()
            if g in others:
                @pl.when(tm == 0)
                def _():
                    across(g, o)

    def relay(g):
        for o in range(2):
            sends, relays = slot_gathers[g][o]
            for kind, d, copy in sends:
                if kind == o:
                    copy.wait_recv()
                    for dd, forward in relays:
                        if dd == d:
                            if g in others:
                                @pl.when(tm > 0)
                                def _():
                                    forward.start()
                            else:
                                forward.start()

    def own_total(g):
        f, span, _, _ = spans[g]
        total = part[f, :, span, jy, ix]
        if blocks:
            drain(arrived.at[:, f, :, span], rs_recv.at[g])
        for k in range(len(blocks)):
            total = total + arrived[k, f, :, span]
        ext[1 + f, jy, ix, :, span] = total

    def up(c, src, step):
        dst = ext.at[0, jy, ix, :, c]
        return remote(src, dst, z_send.at[step - 1], z_recv.at[0, c], {"tm": tm + step})

    def side(c):
        return remote(ext.at[1, jy, ix, :, c], extra.at[c], z_send.at[0], z_recv.at[1, c], {"tm": tm + 1})

    def send_up(c, src, steps=(2, 1)):
        for step in (k for k in steps if k < steps_tm):
            @pl.when(tm < steps_tm - step)
            def _():
                up(c, src, step).start()

    def early(c):
        ref = ext.at[0, jy, ix, :, c]
        return [remote(ref, ref, early_send, early_recv, at(j, i)) for j, i in blocks]

    def earlier(c):
        up(c, extra.at[c], 1).wait_recv()

        @pl.when(even)
        def _():
            side(c).wait_recv()
            total = ext[0, jy, ix, :, c] + extra[c]
            ext[0, jy, ix, :, c] = total
            passing[c] = total + ext[1, jy, ix, :, c]
            send_up(c, passing.at[c])

    def share_earlier(c):
        for copy in early(c):
            copy.start()

    for g in totals:
        c = spans[g][2]
        own_total(g)

        @pl.when(tm == 0)
        def _():
            send_up(c, ext.at[1, jy, ix, :, c])

        @pl.when((tm % 2 == 1) & (tm < steps_tm - 1))
        def _():
            side(c).start()

        share(g)
    chunks = list(range(CHUNKS))
    early_planes, last_planes = (tm == 1) | ((tm > 0) & even), (tm > 1) & (tm % 2 == 1)

    def take(planes, n):
        @pl.when(planes)
        def _():
            for c in chunks[n * CHUNKS // len(others):(n + 1) * CHUNKS // len(others)]:
                earlier(c)
                share_earlier(c)

    for n, g in enumerate(others):
        own_total(g)
        share(g)
        take(early_planes, n)
    for g in totals:
        relay(g)
    for n, g in enumerate(others):
        take(last_planes, n)
        relay(g)

    @pl.when(tm == 0)
    def _():
        ext[0] = jnp.zeros(ext.shape[1:], jnp.float32)

    @pl.when(tm > 0)
    def _():
        if blocks:
            drain(arrived.at[:, 0], early_recv)

    rest = pl.ds(2, slots - 1)
    if outer > 1:
        drain(ext.at[1, pl.ds(0, outer - 1), :, 0], end_recv.at[0, 0])
        drain(ext.at[rest, pl.ds(0, outer - 1), 0, 0], end_recv.at[0, 1])
    if inner > 1:
        drain(ext.at[1, :, pl.ds(0, inner - 1), 1], end_recv.at[1, 0])
        drain(ext.at[rest, 0, pl.ds(0, inner - 1), 1], end_recv.at[1, 1])

    windows = out.shape[0]
    local = [index[w] - tm * slots for w in range(windows)]
    shares = [[jnp.where(local[w] > t, 1.0, jnp.where(local[w] == t, weight[w], 0.0))
               for t in range(slots)] for w in range(windows)]
    factors = [[share[-1]] + [share[t] - share[-1] for t in range(slots - 1)] for share in shares]

    def blend(j, i, o):
        for w in range(windows):
            total = ext[0, j, i, o] + factors[w][0] * ext[1, j, i, o]
            for t in range(1, slots):
                total = total + factors[w][t] * ext[1 + t, j, i, o]
            out[w, j, i, o] = total

    def blend_over(targets):
        for j, i in targets:
            def step(o, carry):
                blend(j, i, o)
                return carry

            lax.fori_loop(0, 2, step, 0)

    blend_over([(outer_peer(e), inner_peer(d)) for e, d in offsets if e == 0 or d == 0])
    @pl.when(tm < steps_tm - 1)
    def _():
        drain(passing, z_send.at[0])

    @pl.when(even & (tm < steps_tm - 2))
    def _():
        drain(passing, z_send.at[1])

    for copy in halos:
        copy.wait_send()
    if blocks:
        drain(arrived, rs_send)
        drain(arrived, ag_send)

    @pl.when(tm > 0)
    def _():
        if blocks:
            drain(arrived.at[:, 0], early_send)

    if inner > 1 and outer > 1:
        for o in range(2):
            drain(ext.at[rest, pl.ds(0, outer - 1), pl.ds(0, inner - 1), o], end_recv.at[o, 2])
        blend_over([blocks[k] for k in far_ks])


def store(held, out, sem):
    size = held.shape[1] // STORES
    for n in range(STORES):
        span = pl.ds(n * size, size)
        pltpu.make_async_copy(held.at[:, span], out.at[:, span], sem).start()
    drain(held, sem)


def binomial_rings(size):
    column = np.zeros(size)
    column[0] += 1.0 - 4.0 * diffusion
    column[1 % size] += diffusion
    column[-1 % size] += diffusion
    ring = np.stack([np.roll(column, x) for x in range(size)], axis=1)
    return [[math.comb(SMOOTH, k) * diffusion ** k * float(x) for x in np.linalg.matrix_power(ring, SMOOTH - k)[0]]
            for k in range(SMOOTH + 1)]


def pieces_of(slots):
    n = max(CHUNKS // 2, 1)
    return [(0, c, 1) for c in range(CHUNKS)] + [(f, c, n) for f in range(1, slots) for c in range(0, CHUNKS, n)]


def rows_view(x, nx, gy):
    lead = x.shape[:-2]
    x = x.reshape(lead + (nx, gy // LANES, LANES))
    x = jnp.swapaxes(x, -3, -2)
    return x


def per_device(control, vertical_modes, mode_counts, perturbations, slot_index, blend_weight):
    members, slots, levels, nx, gy = perturbations.shape
    modes_n = control.shape[1]
    halves = gy // LANES
    level_rows = nx * halves
    tiles, n_mem, steps_tm = lax.axis_size("tile"), lax.axis_size("mem"), lax.axis_size("tm")
    inner = 2 if n_mem % 2 == 0 else 1
    outer = n_mem // inner
    parts = 2 * CHUNKS
    rows = levels // (n_mem * parts) * level_rows
    assert nx >= SMOOTH and level_rows == 8 and rows % 16 == 0
    norm = 1.0 / math.sqrt(members * n_mem - 1)
    fields = members * modes_n
    c = rows_view(control, nx, gy).reshape(fields, level_rows, LANES)
    q = rows_view(perturbations, nx, gy).reshape(members, slots, outer, inner, 2, CHUNKS, rows, LANES)
    dims = (members, slots, modes_n, nx, halves, outer, inner, rows, tiles, steps_tm, norm)
    f32 = jnp.float32
    n_in, n_out = max(inner - 1, 1), max(outer - 1, 1)
    n_pieces = len(pieces_of(slots))
    sides = 2 if tiles > 2 else 1
    dma = pltpu.SemaphoreType.DMA
    windows = slot_index.shape[0]
    held = pl.pallas_call(
        functools.partial(kernel, dims),
        out_shape=pltpu.VMEM((windows, outer, inner, 2, CHUNKS, rows, LANES), f32),
        in_specs=[
            pl.BlockSpec(memory_space=pltpu.HBM),
            pl.BlockSpec(memory_space=pltpu.HBM),
            pl.BlockSpec(memory_space=pltpu.HBM),
            pl.BlockSpec(memory_space=pltpu.HBM),
            pl.BlockSpec(memory_space=pltpu.HBM),
            pl.BlockSpec(memory_space=pltpu.HBM),
        ],
        out_specs=pl.BlockSpec(memory_space=pltpu.VMEM),
        scratch_shapes=[
            pltpu.VMEM((slots + 1, outer, inner, 2, CHUNKS, rows, LANES), f32),
            pltpu.VMEM((fields, level_rows, LANES), f32),
            pltpu.VMEM((sides, fields, level_rows, LANES), f32),
            pltpu.VMEM((sides, fields, level_rows, LANES), f32),
            pltpu.VMEM(q.shape, q.dtype),
            pltpu.VMEM((fields, level_rows, LANES), f32),
            pltpu.VMEM((slots, 2, CHUNKS, outer, inner, rows, LANES), f32),
            pltpu.VMEM((max(n_mem - 1, 1), slots, 2, CHUNKS, rows, LANES), f32),
            pltpu.VMEM((CHUNKS, 2, rows, LANES), f32),
            pltpu.VMEM((CHUNKS, 2, rows, LANES), f32),
            pltpu.SMEM((modes_n, levels), f32),
            pltpu.SMEM((nx,), jnp.int32),
            pltpu.SMEM((windows,), jnp.int32),
            pltpu.SMEM((windows,), f32),
            dma((5,)),
            dma((n_mem,)),
            dma((sides,)),
            dma((sides,)),
            dma,
            dma((n_pieces,)),
            dma((2,)),
            dma((2, CHUNKS)),
            dma,
            dma((2, n_pieces, max(n_in, n_out))),
            dma((2, 3)),
            dma,
            dma,
            pltpu.SemaphoreType.REGULAR,
        ],
        compiler_params=pltpu.CompilerParams(
            collective_id=0, has_side_effects=True),
    )(c, q, vertical_modes.T, mode_counts, slot_index, blend_weight)
    held = held.reshape(windows, levels * level_rows, LANES)
    out = pl.pallas_call(
        store,
        out_shape=jax.ShapeDtypeStruct((windows, levels * level_rows, LANES), f32),
        in_specs=[pl.BlockSpec(memory_space=pltpu.VMEM)],
        out_specs=pl.BlockSpec(memory_space=pltpu.HBM),
        scratch_shapes=[dma],
        compiler_params=pltpu.CompilerParams(vmem_limit_bytes=8 << 20),
    )(held)
    out = out.reshape(windows, levels, halves, nx, LANES)
    return jnp.swapaxes(out, 2, 3).reshape(windows, levels, nx, gy)


def solution(mesh):
    placed = (
        P("mem", None, "tile", None),
        P(),
        P("tile"),
        P("mem", "tm", None, "tile", None),
        P("tm"),
        P("tm"),
    )
    return jax.shard_map(
        per_device,
        mesh=mesh,
        in_specs=placed,
        out_specs=P("tm", None, "tile", None),
        check_vma=False,
    )
```

```python
import functools
import math

import jax
import jax.numpy as jnp
import numpy as np
from jax import lax
from jax.experimental import pallas as pl
from jax.experimental.pallas import tpu as pltpu
from jax.sharding import PartitionSpec as P

SMOOTH = 4
CHUNKS = 4
STORES = 8
LANES = 128
MESH = pl.DeviceIdType.MESH

diffusion = 0.24


def drain(ref, sem):
    pltpu.make_async_copy(ref, ref, sem).wait()


def kernel(dims, control, perturbations, modes_in, counts_in, index_in, weight_in, out, ext, own, near, away, pert,
           smooth, part, arrived, extra, passing, modes, counts, index, weight,
           load_sem, pert_sem, halo_send, halo_recv, rs_send, rs_recv, z_send, z_recv, ag_send, hop_recv, end_recv,
           early_send, early_recv, ready):
    members, slots, modes_n, nx, halves, outer, inner, rows, tiles, steps_tm, norm = dims
    tm = lax.axis_index("tm")
    mem = lax.axis_index("mem")
    tile = lax.axis_index("tile")
    jy, ix = mem // inner, mem % inner
    level_rows = nx * halves
    part_levels = rows // level_rows

    def inner_peer(d):
        return (ix + d) % inner

    def outer_peer(d):
        return (jy + d) % outer

    def at(j, i):
        return {"mem": j * inner + i}

    barrier = pltpu.get_barrier_semaphore()
    tile_offsets = sorted({1 % tiles, (tiles - 1) % tiles} - {0})
    expected = len(tile_offsets) + inner - 1 + outer - 1
    for d in tile_offsets:
        pl.semaphore_signal(barrier, inc=1, device_id={"tile": (tile + d) % tiles}, device_id_type=MESH)
    for d in range(1, inner):
        pl.semaphore_signal(barrier, inc=1, device_id=at(jy, inner_peer(d)), device_id_type=MESH)
    for e in range(1, outer):
        pl.semaphore_signal(barrier, inc=1, device_id=at(outer_peer(e), ix), device_id_type=MESH)

    @pl.when(tm > 0)
    def _():
        pl.semaphore_signal(barrier, inc=1, device_id={"tm": tm - 1}, device_id_type=MESH)

    @pl.when(tm < steps_tm - 1)
    def _():
        pl.semaphore_signal(barrier, inc=1, device_id={"tm": tm + 1}, device_id_type=MESH)

    even = tm % 2 == 0

    @pl.when((tm > 1) & even)
    def _():
        pl.semaphore_signal(barrier, inc=1, device_id={"tm": tm - 2}, device_id_type=MESH)

    load_own = pltpu.make_async_copy(control, own, load_sem.at[0])
    load_own.start()
    load_counts = pltpu.make_async_copy(counts_in, counts, load_sem.at[1])
    load_counts.start()
    load_modes = pltpu.make_async_copy(modes_in, modes, load_sem.at[2])
    load_modes.start()
    load_index = pltpu.make_async_copy(index_in, index, load_sem.at[3])
    load_index.start()
    load_weight = pltpu.make_async_copy(weight_in, weight, load_sem.at[4])
    load_weight.start()

    offsets = sorted(((e, d) for e in range(outer) for d in range(inner)), key=lambda ed: ((ed[0] > 0) + (ed[1] > 0) - 1) % 3)
    blocks = [(outer_peer(e), inner_peer(d)) for e, d in offsets]
    pert_loads = []
    for n, (j, i) in enumerate(blocks):
        copy = pltpu.make_async_copy(perturbations.at[:, :, j, i], pert.at[:, :, j, i], pert_sem.at[n])
        copy.start()
        pert_loads.append(copy)

    row = lax.broadcasted_iota(jnp.int32, (1, level_rows, LANES), 1)
    lane = lax.broadcasted_iota(jnp.int32, (1, level_rows, LANES), 2)
    lon, half = row % nx, row // nx
    first_lon, last_lon = lon == 0, lon == nx - 1
    first_lane, last_lane = lane == 0, lane == LANES - 1
    has_next, has_prev = half < halves - 1, half > 0
    back = level_rows - 1

    def after(v):
        return pltpu.roll(v, level_rows - nx, 1)

    def before(v):
        return after(v) if halves == 2 else pltpu.roll(v, nx, 1)

    def spread(left, right):
        east = pltpu.roll(jnp.where(first_lon, before(right), 0.0), back, 1)
        west = pltpu.roll(jnp.where(last_lon, after(left), 0.0), 1, 1)
        return diffusion * (east + west)

    def relax(left, v, right):
        ahead, behind = after(v), before(v)
        east = pltpu.roll(jnp.where(first_lon, before(right), v), back, 1)
        west = pltpu.roll(jnp.where(last_lon, after(left), v), 1, 1)
        up = pltpu.roll(jnp.where(first_lane, jnp.where(has_next, ahead, 0.0), v), LANES - 1, 2)
        down = pltpu.roll(jnp.where(last_lane, jnp.where(has_prev, behind, 0.0), v), 1, 2)
        return (1.0 - 4.0 * diffusion) * v + diffusion * ((east + west) + (up + down))

    def diffuse_pair(v):
        at_step = binomial_rings(2 * nx)

        crossing = (first_lane & has_next) | (last_lane & has_prev)
        powers = [v]
        for _ in range(SMOOTH):
            v = powers[-1]
            edge = jnp.where(crossing, pltpu.roll(v, nx, 1), 0.0)
            above, below = jnp.where(first_lane, edge, v), jnp.where(last_lane, edge, v)
            powers.append(pltpu.roll(above, LANES - 1, 2) + pltpu.roll(below, 1, 2))

        def mix(distance):
            total = None
            for k, term in enumerate(powers):
                if at_step[k][distance] != 0.0:
                    part = at_step[k][distance] * term
                    total = part if total is None else total + part
            return total

        here = [mix(m) for m in range(1, nx + 1)]
        there = [pltpu.roll(u, nx, 1) for u in here[:-1]]
        other = here[-1]
        for m in range(1, nx):
            other = other + pltpu.roll(jnp.where(lon + m < nx, here[nx - m - 1], there[m - 1]), m, 1)

        def centre():
            total = mix(0)
            for m in range(1, nx):
                total = total + pltpu.roll(jnp.where(lon + m < nx, here[m - 1], there[nx - m - 1]), m, 1)
            return total

        return centre, other

    fields = own.shape[0]

    load_own.wait()
    zero = jnp.zeros((1, level_rows, LANES), jnp.float32)

    c = own[...]
    if tiles == 1:
        for _ in range(SMOOTH):
            c = relax(c, c, c)
    elif tiles == 2 and halves == 2:
        centre, away[0] = diffuse_pair(c)
    elif tiles == 2:
        c, o = relax(zero, c, zero), spread(c, c)
        for _ in range(1, SMOOTH):
            c, o = relax(o, c, o), relax(c, o, c)
        away[0] = o
    else:
        c, left, right = relax(zero, c, zero), spread(zero, c), spread(c, zero)
        for _ in range(1, SMOOTH):
            c, left, right = relax(left, c, right), relax(zero, left, c), relax(c, right, zero)
        away[0] = right
        away[1] = left
    if not (tiles == 2 and halves == 2):
        centre = lambda: c

    chain_peers = jnp.where(tm > 0, 1, 0) + jnp.where(tm < steps_tm - 1, 1, 0)
    chain_peers = chain_peers + jnp.where(even & (tm < steps_tm - 2), 1, 0)
    pl.semaphore_wait(barrier, expected + chain_peers)

    for d in range(1, inner):
        pl.semaphore_signal(ready, inc=1, device_id=at(jy, inner_peer(d)), device_id_type=MESH)

    halos = []
    for n, d in enumerate(tile_offsets):
        copy = pltpu.make_async_remote_copy(
            src_ref=away.at[n], dst_ref=near.at[n], send_sem=halo_send.at[n], recv_sem=halo_recv.at[n],
            device_id={"tile": (tile + d) % tiles}, device_id_type=MESH)
        copy.start()
        halos.append(copy)
    smooth[...] = centre()

    load_counts.wait()
    load_modes.wait()
    load_index.wait()
    load_weight.wait()
    count = jnp.zeros((1, level_rows, LANES), jnp.int32)
    for x in range(nx):
        count = jnp.where(lon == x, counts[x], count)
    for copy in halos:
        copy.wait_recv()
    total = smooth[...]
    for n in range(len(tile_offsets)):
        total = total + near[n]
    mode = lax.broadcasted_iota(jnp.int32, (fields, level_rows, LANES), 0) % modes_n
    smooth[...] = jnp.where(mode < count, total * norm, 0.0)

    pair = 2 * level_rows

    def sums(o, c, j, i, u):
        base = (((j * inner + i) * 2 + o) * CHUNKS + c) * part_levels + 2 * u
        sizes = []
        for t in range(slots):
            acc = [[None] * 2 for _ in range(modes_n)]
            for k in range(members):
                x = pert[k, t, j, i, o, c, pl.ds(pl.multiple_of(u * pair, pair), pair), :].astype(jnp.float32)
                for m in range(modes_n):
                    s = smooth[k * modes_n + m]
                    for v in range(2):
                        term = s * x[v * level_rows:(v + 1) * level_rows]
                        acc[m][v] = term if k == 0 else acc[m][v] + term
            for v in range(2):
                total = modes[0, base + v] * acc[0][v]
                for m in range(1, modes_n):
                    total = total + modes[m, base + v] * acc[m][v]
                place = pl.ds(pl.multiple_of(u * pair + v * level_rows, level_rows), level_rows)
                if t < slots - 1:
                    part[1 + t, o, c, j, i, place, :] = total
                if t == 0:
                    sizes.append(total)
                else:
                    sizes[v] = sizes[v] + total
                if t == slots - 1:
                    part[0, o, c, j, i, place, :] = sizes[v]

    pairs = rows // pair

    def sums_over(count, place):
        def body(n, carry):
            u, n = n % pairs, n // pairs
            sums(*place(n), u)
            return carry

        lax.fori_loop(0, count * pairs, body, 0)

    def remote(src, dst, send, recv, to):
        return pltpu.make_async_remote_copy(
            src_ref=src, dst_ref=dst, send_sem=send, recv_sem=recv, device_id=to, device_id_type=MESH)

    steps_in, steps_out = range(1, inner), range(1, outer)
    pieces = pieces_of(slots)
    spans = [(f, pl.ds(c, n), c, n) for f, c, n in pieces]
    totals = [g for g, (f, _, _) in enumerate(pieces) if f == 0]
    others = [g for g, (f, _, _) in enumerate(pieces) if f > 0]

    blocks = blocks[:-1]
    scatter = [[remote(part.at[f, :, span, j, i], arrived.at[k, f, :, span], rs_send, rs_recv.at[g], at(j, i))
                for k, (j, i) in enumerate(blocks)] for g, (f, span, _, _) in enumerate(spans)]

    near_ks = [k for k, (e, d) in enumerate(offsets[:-1]) if e == 0 or d == 0]
    far_ks = [k for k in range(len(blocks)) if k not in near_ks]
    for ks in (near_ks, far_ks):
        for g in totals:
            c = spans[g][2]
            for k in ks:
                j, i = blocks[k]
                if g == 0:
                    pert_loads[k].wait()
                sums_over(2, lambda n: (n, c, j, i))
                if g == 0 and far_ks and k == far_ks[0]:
                    pl.semaphore_wait(ready, inner - 1)
                scatter[g][k].start()
    for g in others:
        for copy in scatter[g]:
            copy.start()
    pert_loads[-1].wait()
    sums_over(2 * CHUNKS, lambda n: (n % 2, n // 2, jy, ix))

    def last_kind(f, kind):
        return 0 if f == 0 else 1 + (kind == 2)

    def gathers(g, o):
        f, span, _, _ = spans[g]
        sends, relays = [], []

        def move(j, i, to, kind, n):
            ref = ext.at[1 + f, j, i, o, span]
            return remote(ref, ref, ag_send, hop_recv.at[o, g, n] if kind == o else end_recv.at[o, last_kind(f, kind)], to)

        for d in steps_in:
            sends.append((0, d, move(jy, ix, at(jy, inner_peer(d)), 0, d - 1)))
        for e in steps_out:
            sends.append((1, e, move(jy, ix, at(outer_peer(e), ix), 1, e - 1)))
        for d in steps_in:
            for e in steps_out:
                if o == 0:
                    relays.append((d, move(jy, inner_peer(inner - d), at(outer_peer(e), ix), 2, n)))
                else:
                    relays.append((e, move(outer_peer(outer - e), ix, at(jy, inner_peer(d)), 2, n)))
        return sends, relays

    slot_gathers = [[gathers(g, o) for o in range(2)] for g in range(len(pieces))]

    def across(g, o):
        f, span, _, _ = spans[g]
        ref = ext.at[1 + f, jy, ix, o, span]
        for d in steps_in:
            for e in steps_out:
                remote(ref, ref, ag_send, end_recv.at[o, last_kind(f, 2)], at(outer_peer(e), inner_peer(d))).start()

    def urgent(k):
        j, i = blocks[k]
        return (j == 0) & (i == 0)

    first_far = functools.reduce(jnp.logical_or, [urgent(k) for k in far_ks]) if far_ks else tm < 0

    def share(g):
        for o in range(2):
            for _, _, copy in slot_gathers[g][o][0]:
                copy.start()
            if g in others:
                @pl.when((tm == 0) & first_far)
                def _():
                    across(g, o)

    def share_last():
        @pl.when((tm == 0) & jnp.logical_not(first_far))
        def _():
            for g in others:
                for o in range(2):
                    across(g, o)

        @pl.when((tm > 0) & jnp.logical_not(first_far))
        def _():
            for c in range(CHUNKS):
                for copy in early(c, far_ks):
                    copy.start()

    def relay(g):
        for o in range(2):
            sends, relays = slot_gathers[g][o]
            for kind, d, copy in sends:
                if kind == o:
                    copy.wait_recv()
                    for dd, forward in relays:
                        if dd == d:
                            if g in others:
                                @pl.when(tm > 0)
                                def _():
                                    forward.start()
                            else:
                                forward.start()

    def own_total(g):
        f, span, _, _ = spans[g]
        total = part[f, :, span, jy, ix]
        if blocks:
            drain(arrived.at[:, f, :, span], rs_recv.at[g])
        for k in range(len(blocks)):
            total = total + arrived[k, f, :, span]
        ext[1 + f, jy, ix, :, span] = total

    def up(c, src, step):
        dst = ext.at[0, jy, ix, :, c]
        return remote(src, dst, z_send.at[step - 1], z_recv.at[c], {"tm": tm + step})

    def side(c):
        return remote(ext.at[1, jy, ix, :, c], extra.at[c], z_send.at[0], z_recv.at[c], {"tm": tm + 1})

    def send_up(c, src, steps=(2, 1)):
        for step in (k for k in steps if k < steps_tm):
            @pl.when(tm < steps_tm - step)
            def _():
                up(c, src, step).start()

    def early(c, ks):
        ref = ext.at[0, jy, ix, :, c]
        return [remote(ref, ref, early_send, early_recv.at[int(k in far_ks)], at(*blocks[k])) for k in ks]

    def earlier(c):
        @pl.when(jnp.logical_not(even))
        def _():
            up(c, extra.at[c], 1).wait_recv()

        @pl.when(even)
        def _():
            drain(ext.at[pl.ds(0, 2), jy, ix, :, c], z_recv.at[c])
            total = ext[0, jy, ix, :, c] + extra[c]
            ext[0, jy, ix, :, c] = total
            passing[c] = total + ext[1, jy, ix, :, c]
            send_up(c, passing.at[c])

    def share_earlier(c):
        if far_ks:
            @pl.when(first_far)
            def _():
                for copy in early(c, far_ks):
                    copy.start()
        for copy in early(c, near_ks):
            copy.start()

    for g in totals:
        c = spans[g][2]
        own_total(g)

        @pl.when(tm == 0)
        def _():
            send_up(c, ext.at[1, jy, ix, :, c])

        @pl.when((tm % 2 == 1) & (tm < steps_tm - 1))
        def _():
            side(c).start()

        share(g)
    chunks = list(range(CHUNKS))
    early_planes, last_planes = (tm == 1) | ((tm > 0) & even), (tm > 1) & (tm % 2 == 1)

    def take(planes, n):
        @pl.when(planes)
        def _():
            for c in chunks[n * CHUNKS // len(others):(n + 1) * CHUNKS // len(others)]:
                earlier(c)
                share_earlier(c)

    for n, g in enumerate(others):
        own_total(g)
        share(g)
        take(early_planes, n)
    for g in totals:
        relay(g)
    for n, g in enumerate(others):
        take(last_planes, n)
        if n == len(others) - 1:
            share_last()
        relay(g)

    @pl.when(tm == 0)
    def _():
        ext[0] = jnp.zeros(ext.shape[1:], jnp.float32)

    @pl.when(tm > 0)
    def _():
        if near_ks:
            drain(arrived.at[pl.ds(0, len(near_ks)), 0], early_recv.at[0])

    rest = pl.ds(2, slots - 1)
    if outer > 1:
        drain(ext.at[1, pl.ds(0, outer - 1), :, 0], end_recv.at[0, 0])
        drain(ext.at[rest, pl.ds(0, outer - 1), 0, 0], end_recv.at[0, 1])
    if inner > 1:
        drain(ext.at[1, :, pl.ds(0, inner - 1), 1], end_recv.at[1, 0])
        drain(ext.at[rest, 0, pl.ds(0, inner - 1), 1], end_recv.at[1, 1])

    windows = out.shape[0]
    local = [index[w] - tm * slots for w in range(windows)]
    shares = [[jnp.where(local[w] > t, 1.0, jnp.where(local[w] == t, weight[w], 0.0))
               for t in range(slots)] for w in range(windows)]
    factors = [[share[-1]] + [share[t] - share[-1] for t in range(slots - 1)] for share in shares]

    def blend(j, i, o):
        for w in range(windows):
            total = ext[0, j, i, o] + factors[w][0] * ext[1, j, i, o]
            for t in range(1, slots):
                total = total + factors[w][t] * ext[1 + t, j, i, o]
            out[w, j, i, o] = total

    def blend_over(targets):
        for j, i in targets:
            def step(o, carry):
                blend(j, i, o)
                return carry

            lax.fori_loop(0, 2, step, 0)

    blend_over([(outer_peer(e), inner_peer(d)) for e, d in offsets if e == 0 or d == 0])
    @pl.when(tm < steps_tm - 1)
    def _():
        drain(passing, z_send.at[0])

    @pl.when(even & (tm < steps_tm - 2))
    def _():
        drain(passing, z_send.at[1])

    for copy in halos:
        copy.wait_send()
    if blocks:
        drain(arrived, rs_send)
        drain(arrived, ag_send)

    @pl.when(tm > 0)
    def _():
        if blocks:
            drain(arrived.at[:, 0], early_send)

    if inner > 1 and outer > 1:
        @pl.when(tm > 0)
        def _():
            drain(arrived.at[pl.ds(len(near_ks), len(far_ks)), 0], early_recv.at[1])

        for o in range(2):
            drain(ext.at[rest, pl.ds(0, outer - 1), pl.ds(0, inner - 1), o], end_recv.at[o, 2])
        blend_over([blocks[k] for k in far_ks])


def store(held, out, sem):
    size = held.shape[1] // STORES
    for n in range(STORES):
        span = pl.ds(n * size, size)
        pltpu.make_async_copy(held.at[:, span], out.at[:, span], sem).start()
    drain(held, sem)


def binomial_rings(size):
    column = np.zeros(size)
    column[0] += 1.0 - 4.0 * diffusion
    column[1 % size] += diffusion
    column[-1 % size] += diffusion
    ring = np.stack([np.roll(column, x) for x in range(size)], axis=1)
    return [[math.comb(SMOOTH, k) * diffusion ** k * float(x) for x in np.linalg.matrix_power(ring, SMOOTH - k)[0]]
            for k in range(SMOOTH + 1)]


def pieces_of(slots):
    n = max(CHUNKS // 2, 1)
    return [(0, c, 1) for c in range(CHUNKS)] + [(f, c, n) for f in range(1, slots) for c in range(0, CHUNKS, n)]


def rows_view(x, nx, gy):
    lead = x.shape[:-2]
    x = x.reshape(lead + (nx, gy // LANES, LANES))
    x = jnp.swapaxes(x, -3, -2)
    return x


def per_device(control, vertical_modes, mode_counts, perturbations, slot_index, blend_weight):
    members, slots, levels, nx, gy = perturbations.shape
    modes_n = control.shape[1]
    halves = gy // LANES
    level_rows = nx * halves
    tiles, n_mem, steps_tm = lax.axis_size("tile"), lax.axis_size("mem"), lax.axis_size("tm")
    inner = 2 if n_mem % 2 == 0 else 1
    outer = n_mem // inner
    parts = 2 * CHUNKS
    rows = levels // (n_mem * parts) * level_rows
    assert nx >= SMOOTH and level_rows == 8 and rows % 16 == 0
    norm = 1.0 / math.sqrt(members * n_mem - 1)
    fields = members * modes_n
    c = rows_view(control, nx, gy).reshape(fields, level_rows, LANES)
    q = rows_view(perturbations, nx, gy).reshape(members, slots, outer, inner, 2, CHUNKS, rows, LANES)
    dims = (members, slots, modes_n, nx, halves, outer, inner, rows, tiles, steps_tm, norm)
    f32 = jnp.float32
    n_in, n_out = max(inner - 1, 1), max(outer - 1, 1)
    n_pieces = len(pieces_of(slots))
    sides = 2 if tiles > 2 else 1
    dma = pltpu.SemaphoreType.DMA
    windows = slot_index.shape[0]
    held = pl.pallas_call(
        functools.partial(kernel, dims),
        out_shape=pltpu.VMEM((windows, outer, inner, 2, CHUNKS, rows, LANES), f32),
        in_specs=[
            pl.BlockSpec(memory_space=pltpu.HBM),
            pl.BlockSpec(memory_space=pltpu.HBM),
            pl.BlockSpec(memory_space=pltpu.HBM),
            pl.BlockSpec(memory_space=pltpu.HBM),
            pl.BlockSpec(memory_space=pltpu.HBM),
            pl.BlockSpec(memory_space=pltpu.HBM),
        ],
        out_specs=pl.BlockSpec(memory_space=pltpu.VMEM),
        scratch_shapes=[
            pltpu.VMEM((slots + 1, outer, inner, 2, CHUNKS, rows, LANES), f32),
            pltpu.VMEM((fields, level_rows, LANES), f32),
            pltpu.VMEM((sides, fields, level_rows, LANES), f32),
            pltpu.VMEM((sides, fields, level_rows, LANES), f32),
            pltpu.VMEM(q.shape, q.dtype),
            pltpu.VMEM((fields, level_rows, LANES), f32),
            pltpu.VMEM((slots, 2, CHUNKS, outer, inner, rows, LANES), f32),
            pltpu.VMEM((max(n_mem - 1, 1), slots, 2, CHUNKS, rows, LANES), f32),
            pltpu.VMEM((CHUNKS, 2, rows, LANES), f32),
            pltpu.VMEM((CHUNKS, 2, rows, LANES), f32),
            pltpu.SMEM((modes_n, levels), f32),
            pltpu.SMEM((nx,), jnp.int32),
            pltpu.SMEM((windows,), jnp.int32),
            pltpu.SMEM((windows,), f32),
            dma((5,)),
            dma((n_mem,)),
            dma((sides,)),
            dma((sides,)),
            dma,
            dma((n_pieces,)),
            dma((2,)),
            dma((CHUNKS,)),
            dma,
            dma((2, n_pieces, max(n_in, n_out))),
            dma((2, 3)),
            dma,
            dma((2,)),
            pltpu.SemaphoreType.REGULAR,
        ],
        compiler_params=pltpu.CompilerParams(
            collective_id=0, has_side_effects=True),
    )(c, q, vertical_modes.T, mode_counts, slot_index, blend_weight)
    held = held.reshape(windows, levels * level_rows, LANES)
    out = pl.pallas_call(
        store,
        out_shape=jax.ShapeDtypeStruct((windows, levels * level_rows, LANES), f32),
        in_specs=[pl.BlockSpec(memory_space=pltpu.VMEM)],
        out_specs=pl.BlockSpec(memory_space=pltpu.HBM),
        scratch_shapes=[dma],
        compiler_params=pltpu.CompilerParams(vmem_limit_bytes=8 << 20),
    )(held)
    out = out.reshape(windows, levels, halves, nx, LANES)
    return jnp.swapaxes(out, 2, 3).reshape(windows, levels, nx, gy)


def solution(mesh):
    placed = (
        P("mem", None, "tile", None),
        P(),
        P("tile"),
        P("mem", "tm", None, "tile", None),
        P("tm"),
        P("tm"),
    )
    return jax.shard_map(
        per_device,
        mesh=mesh,
        in_specs=placed,
        out_specs=P("tm", None, "tile", None),
        check_vma=False,
    )
```

```python
import functools
import math

import jax
import jax.numpy as jnp
import numpy as np
from jax import lax
from jax.experimental import pallas as pl
from jax.experimental.pallas import tpu as pltpu
from jax.sharding import PartitionSpec as P

SMOOTH = 4
CHUNKS = 4
STORES = 8
LANES = 128
MESH = pl.DeviceIdType.MESH

diffusion = 0.24


def drain(ref, sem):
    pltpu.make_async_copy(ref, ref, sem).wait()


def kernel(dims, control, perturbations, modes_in, counts_in, index_in, weight_in, out, ext, own, near, away, pert,
           smooth, part, arrived, extra, passing, modes, counts, index, weight,
           load_sem, pert_sem, halo_send, halo_recv, rs_send, rs_recv, z_send, z_recv, ag_send, hop_recv, end_recv,
           early_send, early_recv, ready):
    members, slots, modes_n, nx, halves, outer, inner, rows, tiles, steps_tm, norm = dims
    tm = lax.axis_index("tm")
    mem = lax.axis_index("mem")
    tile = lax.axis_index("tile")
    jy, ix = mem // inner, mem % inner
    level_rows = nx * halves
    part_levels = rows // level_rows

    def inner_peer(d):
        return (ix + d) % inner

    def outer_peer(d):
        return (jy + d) % outer

    def at(j, i):
        return {"mem": j * inner + i}

    barrier = pltpu.get_barrier_semaphore()
    tile_offsets = sorted({1 % tiles, (tiles - 1) % tiles} - {0})
    expected = len(tile_offsets) + inner - 1 + outer - 1
    for d in tile_offsets:
        pl.semaphore_signal(barrier, inc=1, device_id={"tile": (tile + d) % tiles}, device_id_type=MESH)
    for d in range(1, inner):
        pl.semaphore_signal(barrier, inc=1, device_id=at(jy, inner_peer(d)), device_id_type=MESH)
    for e in range(1, outer):
        pl.semaphore_signal(barrier, inc=1, device_id=at(outer_peer(e), ix), device_id_type=MESH)

    @pl.when(tm > 0)
    def _():
        pl.semaphore_signal(barrier, inc=1, device_id={"tm": tm - 1}, device_id_type=MESH)

    @pl.when(tm < steps_tm - 1)
    def _():
        pl.semaphore_signal(barrier, inc=1, device_id={"tm": tm + 1}, device_id_type=MESH)

    even = tm % 2 == 0

    @pl.when((tm > 1) & even)
    def _():
        pl.semaphore_signal(barrier, inc=1, device_id={"tm": tm - 2}, device_id_type=MESH)

    load_own = pltpu.make_async_copy(control, own, load_sem.at[0])
    load_own.start()
    load_counts = pltpu.make_async_copy(counts_in, counts, load_sem.at[1])
    load_counts.start()
    load_modes = pltpu.make_async_copy(modes_in, modes, load_sem.at[2])
    load_modes.start()
    load_index = pltpu.make_async_copy(index_in, index, load_sem.at[3])
    load_index.start()
    load_weight = pltpu.make_async_copy(weight_in, weight, load_sem.at[4])
    load_weight.start()

    offsets = sorted(((e, d) for e in range(outer) for d in range(inner)), key=lambda ed: ((ed[0] > 0) + (ed[1] > 0) - 1) % 3)
    blocks = [(outer_peer(e), inner_peer(d)) for e, d in offsets]
    pert_loads = []
    for n, (j, i) in enumerate(blocks):
        copy = pltpu.make_async_copy(perturbations.at[:, :, j, i], pert.at[:, :, j, i], pert_sem.at[n])
        copy.start()
        pert_loads.append(copy)

    row = lax.broadcasted_iota(jnp.int32, (1, level_rows, LANES), 1)
    lane = lax.broadcasted_iota(jnp.int32, (1, level_rows, LANES), 2)
    lon, half = row % nx, row // nx
    first_lon, last_lon = lon == 0, lon == nx - 1
    first_lane, last_lane = lane == 0, lane == LANES - 1
    has_next, has_prev = half < halves - 1, half > 0
    back = level_rows - 1

    def after(v):
        return pltpu.roll(v, level_rows - nx, 1)

    def before(v):
        return after(v) if halves == 2 else pltpu.roll(v, nx, 1)

    def spread(left, right):
        east = pltpu.roll(jnp.where(first_lon, before(right), 0.0), back, 1)
        west = pltpu.roll(jnp.where(last_lon, after(left), 0.0), 1, 1)
        return diffusion * (east + west)

    def relax(left, v, right):
        ahead, behind = after(v), before(v)
        east = pltpu.roll(jnp.where(first_lon, before(right), v), back, 1)
        west = pltpu.roll(jnp.where(last_lon, after(left), v), 1, 1)
        up = pltpu.roll(jnp.where(first_lane, jnp.where(has_next, ahead, 0.0), v), LANES - 1, 2)
        down = pltpu.roll(jnp.where(last_lane, jnp.where(has_prev, behind, 0.0), v), 1, 2)
        return (1.0 - 4.0 * diffusion) * v + diffusion * ((east + west) + (up + down))

    def diffuse_pair(v):
        at_step = binomial_rings(2 * nx)

        crossing = (first_lane & has_next) | (last_lane & has_prev)
        powers = [v]
        for _ in range(SMOOTH):
            v = powers[-1]
            edge = jnp.where(crossing, pltpu.roll(v, nx, 1), 0.0)
            above, below = jnp.where(first_lane, edge, v), jnp.where(last_lane, edge, v)
            powers.append(pltpu.roll(above, LANES - 1, 2) + pltpu.roll(below, 1, 2))

        def mix(distance):
            total = None
            for k, term in enumerate(powers):
                if at_step[k][distance] != 0.0:
                    part = at_step[k][distance] * term
                    total = part if total is None else total + part
            return total

        here = [mix(m) for m in range(1, nx + 1)]
        there = [pltpu.roll(u, nx, 1) for u in here[:-1]]
        other = here[-1]
        for m in range(1, nx):
            other = other + pltpu.roll(jnp.where(lon + m < nx, here[nx - m - 1], there[m - 1]), m, 1)

        def centre():
            total = mix(0)
            for m in range(1, nx):
                total = total + pltpu.roll(jnp.where(lon + m < nx, here[m - 1], there[nx - m - 1]), m, 1)
            return total

        return centre, other

    fields = own.shape[0]

    load_own.wait()
    zero = jnp.zeros((1, level_rows, LANES), jnp.float32)

    c = own[...]
    if tiles == 1:
        for _ in range(SMOOTH):
            c = relax(c, c, c)
    elif tiles == 2 and halves == 2:
        centre, away[0] = diffuse_pair(c)
    elif tiles == 2:
        c, o = relax(zero, c, zero), spread(c, c)
        for _ in range(1, SMOOTH):
            c, o = relax(o, c, o), relax(c, o, c)
        away[0] = o
    else:
        c, left, right = relax(zero, c, zero), spread(zero, c), spread(c, zero)
        for _ in range(1, SMOOTH):
            c, left, right = relax(left, c, right), relax(zero, left, c), relax(c, right, zero)
        away[0] = right
        away[1] = left
    if not (tiles == 2 and halves == 2):
        centre = lambda: c

    chain_peers = jnp.where(tm > 0, 1, 0) + jnp.where(tm < steps_tm - 1, 1, 0)
    chain_peers = chain_peers + jnp.where(even & (tm < steps_tm - 2), 1, 0)
    pl.semaphore_wait(barrier, expected + chain_peers)

    for d in range(1, inner):
        pl.semaphore_signal(ready, inc=1, device_id=at(jy, inner_peer(d)), device_id_type=MESH)

    halos = []
    for n, d in enumerate(tile_offsets):
        copy = pltpu.make_async_remote_copy(
            src_ref=away.at[n], dst_ref=near.at[n], send_sem=halo_send.at[n], recv_sem=halo_recv.at[n],
            device_id={"tile": (tile + d) % tiles}, device_id_type=MESH)
        copy.start()
        halos.append(copy)
    smooth[...] = centre()

    load_counts.wait()
    load_modes.wait()
    load_index.wait()
    load_weight.wait()
    count = jnp.zeros((1, level_rows, LANES), jnp.int32)
    for x in range(nx):
        count = jnp.where(lon == x, counts[x], count)
    for copy in halos:
        copy.wait_recv()
    total = smooth[...]
    for n in range(len(tile_offsets)):
        total = total + near[n]
    mode = lax.broadcasted_iota(jnp.int32, (fields, level_rows, LANES), 0) % modes_n
    smooth[...] = jnp.where(mode < count, total * norm, 0.0)

    pair = 2 * level_rows

    def sums(o, c, j, i, u):
        base = (((j * inner + i) * 2 + o) * CHUNKS + c) * part_levels + 2 * u
        sizes = []
        for t in range(slots):
            acc = [[None] * 2 for _ in range(modes_n)]
            for k in range(members):
                x = pert[k, t, j, i, o, c, pl.ds(pl.multiple_of(u * pair, pair), pair), :].astype(jnp.float32)
                for m in range(modes_n):
                    s = smooth[k * modes_n + m]
                    for v in range(2):
                        term = s * x[v * level_rows:(v + 1) * level_rows]
                        acc[m][v] = term if k == 0 else acc[m][v] + term
            for v in range(2):
                total = modes[0, base + v] * acc[0][v]
                for m in range(1, modes_n):
                    total = total + modes[m, base + v] * acc[m][v]
                place = pl.ds(pl.multiple_of(u * pair + v * level_rows, level_rows), level_rows)
                if t < slots - 1:
                    part[1 + t, o, c, j, i, place, :] = total
                if t == 0:
                    sizes.append(total)
                else:
                    sizes[v] = sizes[v] + total
                if t == slots - 1:
                    part[0, o, c, j, i, place, :] = sizes[v]

    pairs = rows // pair

    def sums_over(count, place):
        def body(n, carry):
            u, n = n % pairs, n // pairs
            sums(*place(n), u)
            return carry

        lax.fori_loop(0, count * pairs, body, 0)

    def remote(src, dst, send, recv, to):
        return pltpu.make_async_remote_copy(
            src_ref=src, dst_ref=dst, send_sem=send, recv_sem=recv, device_id=to, device_id_type=MESH)

    steps_in, steps_out = range(1, inner), range(1, outer)
    pieces = pieces_of(slots)
    spans = [(f, pl.ds(c, n), c, n) for f, c, n in pieces]
    totals = [g for g, (f, _, _) in enumerate(pieces) if f == 0]
    others = [g for g, (f, _, _) in enumerate(pieces) if f > 0]

    blocks = blocks[:-1]
    scatter = [[remote(part.at[f, :, span, j, i], arrived.at[k, f, :, span], rs_send, rs_recv.at[g], at(j, i))
                for k, (j, i) in enumerate(blocks)] for g, (f, span, _, _) in enumerate(spans)]

    near_ks = [k for k, (e, d) in enumerate(offsets[:-1]) if e == 0 or d == 0]
    far_ks = [k for k in range(len(blocks)) if k not in near_ks]
    for ks in (near_ks, far_ks):
        for g in totals:
            c = spans[g][2]
            for k in ks:
                j, i = blocks[k]
                if g == 0:
                    pert_loads[k].wait()
                sums_over(2, lambda n: (n, c, j, i))
                if g == 0 and far_ks and k == far_ks[0]:
                    pl.semaphore_wait(ready, inner - 1)
                scatter[g][k].start()
    for g in others:
        for copy in scatter[g]:
            copy.start()
    pert_loads[-1].wait()
    sums_over(2 * CHUNKS, lambda n: (n % 2, n // 2, jy, ix))

    def last_kind(f, kind):
        return 0 if f == 0 else 1 + (kind == 2)

    def gathers(g, o):
        f, span, _, _ = spans[g]
        sends, relays = [], []

        def move(j, i, to, kind, n):
            ref = ext.at[1 + f, j, i, o, span]
            return remote(ref, ref, ag_send, hop_recv.at[o, g, n] if kind == o else end_recv.at[o, last_kind(f, kind)], to)

        for d in steps_in:
            sends.append((0, d, move(jy, ix, at(jy, inner_peer(d)), 0, d - 1)))
        for e in steps_out:
            sends.append((1, e, move(jy, ix, at(outer_peer(e), ix), 1, e - 1)))
        for d in steps_in:
            for e in steps_out:
                if o == 0:
                    relays.append((d, move(jy, inner_peer(inner - d), at(outer_peer(e), ix), 2, n)))
                else:
                    relays.append((e, move(outer_peer(outer - e), ix, at(jy, inner_peer(d)), 2, n)))
        return sends, relays

    slot_gathers = [[gathers(g, o) for o in range(2)] for g in range(len(pieces))]

    def across(g, o):
        f, span, _, _ = spans[g]
        ref = ext.at[1 + f, jy, ix, o, span]
        for d in steps_in:
            for e in steps_out:
                remote(ref, ref, ag_send, end_recv.at[o, last_kind(f, 2)], at(outer_peer(e), inner_peer(d))).start()

    def urgent(k):
        j, i = blocks[k]
        return (j == 0) & (i == 0)

    first_far = functools.reduce(jnp.logical_or, [urgent(k) for k in far_ks]) if far_ks else tm < 0

    def share(g):
        for o in range(2):
            for _, _, copy in slot_gathers[g][o][0]:
                copy.start()
            if g in others:
                @pl.when((tm == 0) & first_far)
                def _():
                    across(g, o)

    def share_last():
        @pl.when((tm == 0) & jnp.logical_not(first_far))
        def _():
            for g in others:
                for o in range(2):
                    across(g, o)

        @pl.when((tm > 0) & jnp.logical_not(first_far))
        def _():
            for c in range(CHUNKS):
                for copy in early(c, far_ks):
                    copy.start()

    def relay(g):
        for o in range(2):
            sends, relays = slot_gathers[g][o]
            for kind, d, copy in sends:
                if kind == o:
                    copy.wait_recv()
                    for dd, forward in relays:
                        if dd == d:
                            if g in others:
                                @pl.when(tm > 0)
                                def _():
                                    forward.start()
                            else:
                                forward.start()

    def own_total(g):
        f, span, _, _ = spans[g]
        total = part[f, :, span, jy, ix]
        if blocks:
            drain(arrived.at[:, f, :, span], rs_recv.at[g])
        for k in range(len(blocks)):
            total = total + arrived[k, f, :, span]
        ext[1 + f, jy, ix, :, span] = total

    def up(c, src, step):
        dst = ext.at[0, jy, ix, :, c]
        return remote(src, dst, z_send.at[step - 1], z_recv.at[c], {"tm": tm + step})

    def side(c):
        return remote(ext.at[1, jy, ix, :, c], extra.at[c], z_send.at[0], z_recv.at[c], {"tm": tm + 1})

    def send_up(c, src, steps=(2, 1)):
        for step in (k for k in steps if k < steps_tm):
            @pl.when(tm < steps_tm - step)
            def _():
                up(c, src, step).start()

    def early(c, ks):
        ref = ext.at[0, jy, ix, :, c]
        return [remote(ref, ref, early_send, early_recv.at[int(k in far_ks)], at(*blocks[k])) for k in ks]

    def earlier(c):
        @pl.when(jnp.logical_not(even))
        def _():
            up(c, extra.at[c], 1).wait_recv()

        @pl.when(even)
        def _():
            drain(ext.at[pl.ds(0, 2), jy, ix, :, c], z_recv.at[c])
            total = ext[0, jy, ix, :, c] + extra[c]
            ext[0, jy, ix, :, c] = total
            passing[c] = total + ext[1, jy, ix, :, c]
            send_up(c, passing.at[c])

    def share_earlier(c):
        if far_ks:
            @pl.when(first_far)
            def _():
                for copy in early(c, far_ks):
                    copy.start()
        for copy in early(c, near_ks):
            copy.start()

    for g in totals:
        c = spans[g][2]
        own_total(g)

        @pl.when(tm == 0)
        def _():
            send_up(c, ext.at[1, jy, ix, :, c], (2,))
            if c > 0:
                send_up(c - 1, ext.at[1, jy, ix, :, c - 1], (1,))
            if c == CHUNKS - 1:
                send_up(c, ext.at[1, jy, ix, :, c], (1,))

        @pl.when((tm % 2 == 1) & (tm < steps_tm - 1))
        def _():
            side(c).start()

        share(g)
    chunks = list(range(CHUNKS))
    early_planes, last_planes = (tm == 1) | ((tm > 0) & even), (tm > 1) & (tm % 2 == 1)

    def take(planes, n):
        @pl.when(planes)
        def _():
            for c in chunks[n * CHUNKS // len(others):(n + 1) * CHUNKS // len(others)]:
                earlier(c)
                share_earlier(c)

    for n, g in enumerate(others):
        own_total(g)
        share(g)
        take(early_planes, n)
    for g in totals:
        relay(g)
    for n, g in enumerate(others):
        take(last_planes, n)
        if n == len(others) - 1:
            share_last()
        relay(g)

    @pl.when(tm == 0)
    def _():
        ext[0] = jnp.zeros(ext.shape[1:], jnp.float32)

    @pl.when(tm > 0)
    def _():
        if near_ks:
            drain(arrived.at[pl.ds(0, len(near_ks)), 0], early_recv.at[0])

    rest = pl.ds(2, slots - 1)
    if outer > 1:
        drain(ext.at[1, pl.ds(0, outer - 1), :, 0], end_recv.at[0, 0])
        drain(ext.at[rest, pl.ds(0, outer - 1), 0, 0], end_recv.at[0, 1])
    if inner > 1:
        drain(ext.at[1, :, pl.ds(0, inner - 1), 1], end_recv.at[1, 0])
        drain(ext.at[rest, 0, pl.ds(0, inner - 1), 1], end_recv.at[1, 1])

    windows = out.shape[0]
    local = [index[w] - tm * slots for w in range(windows)]
    shares = [[jnp.where(local[w] > t, 1.0, jnp.where(local[w] == t, weight[w], 0.0))
               for t in range(slots)] for w in range(windows)]
    factors = [[share[-1]] + [share[t] - share[-1] for t in range(slots - 1)] for share in shares]

    def blend(j, i, o):
        for w in range(windows):
            total = ext[0, j, i, o] + factors[w][0] * ext[1, j, i, o]
            for t in range(1, slots):
                total = total + factors[w][t] * ext[1 + t, j, i, o]
            out[w, j, i, o] = total

    def blend_over(targets):
        for j, i in targets:
            def step(o, carry):
                blend(j, i, o)
                return carry

            lax.fori_loop(0, 2, step, 0)

    blend_over([(outer_peer(e), inner_peer(d)) for e, d in offsets if e == 0 or d == 0])
    @pl.when(tm < steps_tm - 1)
    def _():
        drain(passing, z_send.at[0])

    @pl.when(even & (tm < steps_tm - 2))
    def _():
        drain(passing, z_send.at[1])

    for copy in halos:
        copy.wait_send()
    if blocks:
        drain(arrived, rs_send)
        drain(arrived, ag_send)

    @pl.when(tm > 0)
    def _():
        if blocks:
            drain(arrived.at[:, 0], early_send)

    if inner > 1 and outer > 1:
        @pl.when(tm > 0)
        def _():
            drain(arrived.at[pl.ds(len(near_ks), len(far_ks)), 0], early_recv.at[1])

        for o in range(2):
            drain(ext.at[rest, pl.ds(0, outer - 1), pl.ds(0, inner - 1), o], end_recv.at[o, 2])
        blend_over([blocks[k] for k in far_ks])


def store(held, out, sem):
    size = held.shape[1] // STORES
    for n in range(STORES):
        span = pl.ds(n * size, size)
        pltpu.make_async_copy(held.at[:, span], out.at[:, span], sem).start()
    drain(held, sem)


def binomial_rings(size):
    column = np.zeros(size)
    column[0] += 1.0 - 4.0 * diffusion
    column[1 % size] += diffusion
    column[-1 % size] += diffusion
    ring = np.stack([np.roll(column, x) for x in range(size)], axis=1)
    return [[math.comb(SMOOTH, k) * diffusion ** k * float(x) for x in np.linalg.matrix_power(ring, SMOOTH - k)[0]]
            for k in range(SMOOTH + 1)]


def pieces_of(slots):
    n = max(CHUNKS // 2, 1)
    return [(0, c, 1) for c in range(CHUNKS)] + [(f, c, n) for f in range(1, slots) for c in range(0, CHUNKS, n)]


def rows_view(x, nx, gy):
    lead = x.shape[:-2]
    x = x.reshape(lead + (nx, gy // LANES, LANES))
    x = jnp.swapaxes(x, -3, -2)
    return x


def per_device(control, vertical_modes, mode_counts, perturbations, slot_index, blend_weight):
    members, slots, levels, nx, gy = perturbations.shape
    modes_n = control.shape[1]
    halves = gy // LANES
    level_rows = nx * halves
    tiles, n_mem, steps_tm = lax.axis_size("tile"), lax.axis_size("mem"), lax.axis_size("tm")
    inner = 2 if n_mem % 2 == 0 else 1
    outer = n_mem // inner
    parts = 2 * CHUNKS
    rows = levels // (n_mem * parts) * level_rows
    assert nx >= SMOOTH and level_rows == 8 and rows % 16 == 0
    norm = 1.0 / math.sqrt(members * n_mem - 1)
    fields = members * modes_n
    c = rows_view(control, nx, gy).reshape(fields, level_rows, LANES)
    q = rows_view(perturbations, nx, gy).reshape(members, slots, outer, inner, 2, CHUNKS, rows, LANES)
    dims = (members, slots, modes_n, nx, halves, outer, inner, rows, tiles, steps_tm, norm)
    f32 = jnp.float32
    n_in, n_out = max(inner - 1, 1), max(outer - 1, 1)
    n_pieces = len(pieces_of(slots))
    sides = 2 if tiles > 2 else 1
    dma = pltpu.SemaphoreType.DMA
    windows = slot_index.shape[0]
    held = pl.pallas_call(
        functools.partial(kernel, dims),
        out_shape=pltpu.VMEM((windows, outer, inner, 2, CHUNKS, rows, LANES), f32),
        in_specs=[
            pl.BlockSpec(memory_space=pltpu.HBM),
            pl.BlockSpec(memory_space=pltpu.HBM),
            pl.BlockSpec(memory_space=pltpu.HBM),
            pl.BlockSpec(memory_space=pltpu.HBM),
            pl.BlockSpec(memory_space=pltpu.HBM),
            pl.BlockSpec(memory_space=pltpu.HBM),
        ],
        out_specs=pl.BlockSpec(memory_space=pltpu.VMEM),
        scratch_shapes=[
            pltpu.VMEM((slots + 1, outer, inner, 2, CHUNKS, rows, LANES), f32),
            pltpu.VMEM((fields, level_rows, LANES), f32),
            pltpu.VMEM((sides, fields, level_rows, LANES), f32),
            pltpu.VMEM((sides, fields, level_rows, LANES), f32),
            pltpu.VMEM(q.shape, q.dtype),
            pltpu.VMEM((fields, level_rows, LANES), f32),
            pltpu.VMEM((slots, 2, CHUNKS, outer, inner, rows, LANES), f32),
            pltpu.VMEM((max(n_mem - 1, 1), slots, 2, CHUNKS, rows, LANES), f32),
            pltpu.VMEM((CHUNKS, 2, rows, LANES), f32),
            pltpu.VMEM((CHUNKS, 2, rows, LANES), f32),
            pltpu.SMEM((modes_n, levels), f32),
            pltpu.SMEM((nx,), jnp.int32),
            pltpu.SMEM((windows,), jnp.int32),
            pltpu.SMEM((windows,), f32),
            dma((5,)),
            dma((n_mem,)),
            dma((sides,)),
            dma((sides,)),
            dma,
            dma((n_pieces,)),
            dma((2,)),
            dma((CHUNKS,)),
            dma,
            dma((2, n_pieces, max(n_in, n_out))),
            dma((2, 3)),
            dma,
            dma((2,)),
            pltpu.SemaphoreType.REGULAR,
        ],
        compiler_params=pltpu.CompilerParams(
            collective_id=0, has_side_effects=True),
    )(c, q, vertical_modes.T, mode_counts, slot_index, blend_weight)
    held = held.reshape(windows, levels * level_rows, LANES)
    out = pl.pallas_call(
        store,
        out_shape=jax.ShapeDtypeStruct((windows, levels * level_rows, LANES), f32),
        in_specs=[pl.BlockSpec(memory_space=pltpu.VMEM)],
        out_specs=pl.BlockSpec(memory_space=pltpu.HBM),
        scratch_shapes=[dma],
        compiler_params=pltpu.CompilerParams(vmem_limit_bytes=8 << 20),
    )(held)
    out = out.reshape(windows, levels, halves, nx, LANES)
    return jnp.swapaxes(out, 2, 3).reshape(windows, levels, nx, gy)


def solution(mesh):
    placed = (
        P("mem", None, "tile", None),
        P(),
        P("tile"),
        P("mem", "tm", None, "tile", None),
        P("tm"),
        P("tm"),
    )
    return jax.shard_map(
        per_device,
        mesh=mesh,
        in_specs=placed,
        out_specs=P("tm", None, "tile", None),
        check_vma=False,
    )
```

```python
import functools
import math

import jax
import jax.numpy as jnp
import numpy as np
from jax import lax
from jax.experimental import pallas as pl
from jax.experimental.pallas import tpu as pltpu
from jax.sharding import PartitionSpec as P

SMOOTH = 4
CHUNKS = 4
STORES = 8
LANES = 128
MESH = pl.DeviceIdType.MESH

diffusion = 0.24


def drain(ref, sem):
    pltpu.make_async_copy(ref, ref, sem).wait()


def kernel(dims, control, perturbations, modes_in, counts_in, index_in, weight_in, out, ext, own, near, away, pert,
           smooth, part, arrived, extra, passing, modes, counts, index, weight,
           load_sem, pert_sem, halo_send, halo_recv, rs_send, rs_recv, z_send, z_recv, ag_send, relay_send, across_send, hop_recv, far_recv,
           early_send, early_recv, ready):
    members, slots, modes_n, nx, halves, outer, inner, rows, tiles, steps_tm, norm = dims
    tm = lax.axis_index("tm")
    mem = lax.axis_index("mem")
    tile = lax.axis_index("tile")
    jy, ix = mem // inner, mem % inner
    level_rows = nx * halves
    part_levels = rows // level_rows

    def inner_peer(d):
        return (ix + d) % inner

    def outer_peer(d):
        return (jy + d) % outer

    def at(j, i):
        return {"mem": j * inner + i}

    barrier = pltpu.get_barrier_semaphore()
    tile_offsets = sorted({1 % tiles, (tiles - 1) % tiles} - {0})
    expected = len(tile_offsets) + inner - 1 + outer - 1
    for d in tile_offsets:
        pl.semaphore_signal(barrier, inc=1, device_id={"tile": (tile + d) % tiles}, device_id_type=MESH)
    for d in range(1, inner):
        pl.semaphore_signal(barrier, inc=1, device_id=at(jy, inner_peer(d)), device_id_type=MESH)
    for e in range(1, outer):
        pl.semaphore_signal(barrier, inc=1, device_id=at(outer_peer(e), ix), device_id_type=MESH)

    @pl.when(tm > 0)
    def _():
        pl.semaphore_signal(barrier, inc=1, device_id={"tm": tm - 1}, device_id_type=MESH)

    @pl.when(tm < steps_tm - 1)
    def _():
        pl.semaphore_signal(barrier, inc=1, device_id={"tm": tm + 1}, device_id_type=MESH)

    even = tm % 2 == 0

    @pl.when((tm > 1) & even)
    def _():
        pl.semaphore_signal(barrier, inc=1, device_id={"tm": tm - 2}, device_id_type=MESH)

    load_own = pltpu.make_async_copy(control, own, load_sem.at[0])
    load_own.start()
    load_counts = pltpu.make_async_copy(counts_in, counts, load_sem.at[1])
    load_counts.start()
    load_modes = pltpu.make_async_copy(modes_in, modes, load_sem.at[2])
    load_modes.start()
    load_index = pltpu.make_async_copy(index_in, index, load_sem.at[3])
    load_index.start()
    load_weight = pltpu.make_async_copy(weight_in, weight, load_sem.at[4])
    load_weight.start()

    offsets = sorted(((e, d) for e in range(outer) for d in range(inner)), key=lambda ed: ((ed[0] > 0) + (ed[1] > 0) - 1) % 3)
    blocks = [(outer_peer(e), inner_peer(d)) for e, d in offsets]
    pert_loads = []
    for n, (j, i) in enumerate(blocks):
        copy = pltpu.make_async_copy(perturbations.at[:, :, j, i], pert.at[:, :, j, i], pert_sem.at[n])
        copy.start()
        pert_loads.append(copy)

    row = lax.broadcasted_iota(jnp.int32, (1, level_rows, LANES), 1)
    lane = lax.broadcasted_iota(jnp.int32, (1, level_rows, LANES), 2)
    lon, half = row % nx, row // nx
    first_lon, last_lon = lon == 0, lon == nx - 1
    first_lane, last_lane = lane == 0, lane == LANES - 1
    has_next, has_prev = half < halves - 1, half > 0
    back = level_rows - 1

    def after(v):
        return pltpu.roll(v, level_rows - nx, 1)

    def before(v):
        return after(v) if halves == 2 else pltpu.roll(v, nx, 1)

    def spread(left, right):
        east = pltpu.roll(jnp.where(first_lon, before(right), 0.0), back, 1)
        west = pltpu.roll(jnp.where(last_lon, after(left), 0.0), 1, 1)
        return diffusion * (east + west)

    def relax(left, v, right):
        ahead, behind = after(v), before(v)
        east = pltpu.roll(jnp.where(first_lon, before(right), v), back, 1)
        west = pltpu.roll(jnp.where(last_lon, after(left), v), 1, 1)
        up = pltpu.roll(jnp.where(first_lane, jnp.where(has_next, ahead, 0.0), v), LANES - 1, 2)
        down = pltpu.roll(jnp.where(last_lane, jnp.where(has_prev, behind, 0.0), v), 1, 2)
        return (1.0 - 4.0 * diffusion) * v + diffusion * ((east + west) + (up + down))

    def diffuse_pair(v):
        at_step = binomial_rings(2 * nx)

        crossing = (first_lane & has_next) | (last_lane & has_prev)
        powers = [v]
        for _ in range(SMOOTH):
            v = powers[-1]
            edge = jnp.where(crossing, pltpu.roll(v, nx, 1), 0.0)
            above, below = jnp.where(first_lane, edge, v), jnp.where(last_lane, edge, v)
            powers.append(pltpu.roll(above, LANES - 1, 2) + pltpu.roll(below, 1, 2))

        def mix(distance):
            total = None
            for k, term in enumerate(powers):
                if at_step[k][distance] != 0.0:
                    part = at_step[k][distance] * term
                    total = part if total is None else total + part
            return total

        here = [mix(m) for m in range(1, nx + 1)]
        there = [pltpu.roll(u, nx, 1) for u in here[:-1]]
        other = here[-1]
        for m in range(1, nx):
            other = other + pltpu.roll(jnp.where(lon + m < nx, here[nx - m - 1], there[m - 1]), m, 1)

        def centre():
            total = mix(0)
            for m in range(1, nx):
                total = total + pltpu.roll(jnp.where(lon + m < nx, here[m - 1], there[nx - m - 1]), m, 1)
            return total

        return centre, other

    fields = own.shape[0]

    load_own.wait()
    zero = jnp.zeros((1, level_rows, LANES), jnp.float32)

    c = own[...]
    if tiles == 1:
        for _ in range(SMOOTH):
            c = relax(c, c, c)
    elif tiles == 2 and halves == 2:
        centre, away[0] = diffuse_pair(c)
    elif tiles == 2:
        c, o = relax(zero, c, zero), spread(c, c)
        for _ in range(1, SMOOTH):
            c, o = relax(o, c, o), relax(c, o, c)
        away[0] = o
    else:
        c, left, right = relax(zero, c, zero), spread(zero, c), spread(c, zero)
        for _ in range(1, SMOOTH):
            c, left, right = relax(left, c, right), relax(zero, left, c), relax(c, right, zero)
        away[0] = right
        away[1] = left
    if not (tiles == 2 and halves == 2):
        centre = lambda: c

    chain_peers = jnp.where(tm > 0, 1, 0) + jnp.where(tm < steps_tm - 1, 1, 0)
    chain_peers = chain_peers + jnp.where(even & (tm < steps_tm - 2), 1, 0)
    pl.semaphore_wait(barrier, expected + chain_peers)

    for d in range(1, inner):
        pl.semaphore_signal(ready, inc=1, device_id=at(jy, inner_peer(d)), device_id_type=MESH)

    halos = []
    for n, d in enumerate(tile_offsets):
        copy = pltpu.make_async_remote_copy(
            src_ref=away.at[n], dst_ref=near.at[n], send_sem=halo_send.at[n], recv_sem=halo_recv.at[n],
            device_id={"tile": (tile + d) % tiles}, device_id_type=MESH)
        copy.start()
        halos.append(copy)
    smooth[...] = centre()

    load_counts.wait()
    load_modes.wait()
    load_index.wait()
    load_weight.wait()
    count = jnp.zeros((1, level_rows, LANES), jnp.int32)
    for x in range(nx):
        count = jnp.where(lon == x, counts[x], count)
    for copy in halos:
        copy.wait_recv()
    total = smooth[...]
    for n in range(len(tile_offsets)):
        total = total + near[n]
    mode = lax.broadcasted_iota(jnp.int32, (fields, level_rows, LANES), 0) % modes_n
    smooth[...] = jnp.where(mode < count, total * norm, 0.0)

    pair = 2 * level_rows

    def sums(o, c, j, i, u):
        base = (((j * inner + i) * 2 + o) * CHUNKS + c) * part_levels + 2 * u
        sizes = []
        for t in range(slots):
            acc = [[None] * 2 for _ in range(modes_n)]
            for k in range(members):
                x = pert[k, t, j, i, o, c, pl.ds(pl.multiple_of(u * pair, pair), pair), :].astype(jnp.float32)
                for m in range(modes_n):
                    s = smooth[k * modes_n + m]
                    for v in range(2):
                        term = s * x[v * level_rows:(v + 1) * level_rows]
                        acc[m][v] = term if k == 0 else acc[m][v] + term
            for v in range(2):
                total = modes[0, base + v] * acc[0][v]
                for m in range(1, modes_n):
                    total = total + modes[m, base + v] * acc[m][v]
                place = pl.ds(pl.multiple_of(u * pair + v * level_rows, level_rows), level_rows)
                if t < slots - 1:
                    part[1 + t, o, c, j, i, place, :] = total
                if t == 0:
                    sizes.append(total)
                else:
                    sizes[v] = sizes[v] + total
                if t == slots - 1:
                    part[0, o, c, j, i, place, :] = sizes[v]

    pairs = rows // pair

    def sums_over(count, place):
        def body(n, carry):
            u, n = n % pairs, n // pairs
            sums(*place(n), u)
            return carry

        lax.fori_loop(0, count * pairs, body, 0)

    def remote(src, dst, send, recv, to):
        return pltpu.make_async_remote_copy(
            src_ref=src, dst_ref=dst, send_sem=send, recv_sem=recv, device_id=to, device_id_type=MESH)

    steps_in, steps_out = range(1, inner), range(1, outer)
    pieces = pieces_of(slots)
    spans = [(f, pl.ds(c, n), c, n) for f, c, n in pieces]
    totals = [g for g, (f, _, _) in enumerate(pieces) if f == 0]
    others = [g for g, (f, _, _) in enumerate(pieces) if f > 0]

    blocks = blocks[:-1]
    scatter = [[remote(part.at[f, :, span, j, i], arrived.at[k, f, :, span], rs_send, rs_recv.at[g], at(j, i))
                for k, (j, i) in enumerate(blocks)] for g, (f, span, _, _) in enumerate(spans)]

    near_ks = [k for k, (e, d) in enumerate(offsets[:-1]) if e == 0 or d == 0]
    far_ks = [k for k in range(len(blocks)) if k not in near_ks]
    for ks in (near_ks, far_ks):
        for g in totals:
            c = spans[g][2]
            for k in ks:
                j, i = blocks[k]
                if g == 0:
                    pert_loads[k].wait()
                sums_over(2, lambda n: (n, c, j, i))
                if g == 0 and far_ks and k == far_ks[0]:
                    pl.semaphore_wait(ready, inner - 1)
                scatter[g][k].start()
    for g in others:
        for copy in scatter[g]:
            copy.start()
    pert_loads[-1].wait()
    sums_over(2 * CHUNKS, lambda n: (n % 2, n // 2, jy, ix))

    square = inner == 2 and outer == 2
    first_far = mem == inner * outer - 1 if square else tm < 0

    def near_copies(g):
        f, span, c, _ = spans[g]
        slot = c // 2 if f == 0 else g - len(totals) + CHUNKS // 2
        ref = ext.at[1 + f, jy, ix, :, span]
        return ([remote(ref, ref, ag_send, hop_recv.at[0, slot, d - 1], at(jy, inner_peer(d))) for d in steps_in]
                + [remote(ref, ref, ag_send, hop_recv.at[1, slot, e - 1], at(outer_peer(e), ix)) for e in steps_out])

    def across(g):
        f, span, _, _ = spans[g]
        ref = ext.at[1 + f, jy, ix, :, span]
        for k in far_ks:
            remote(ref, ref, across_send, far_recv.at[min(f, 1)], at(*blocks[k])).start()

    def share(g):
        for copy in near_copies(g):
            copy.start()
        if not square:
            across(g)
        elif g in others:
            @pl.when((tm == 0) & first_far)
            def _():
                across(g)

    def share_last():
        if square:
            @pl.when((tm == 0) & jnp.logical_not(first_far))
            def _():
                for g in others:
                    across(g)

        @pl.when((tm > 0) & jnp.logical_not(first_far))
        def _():
            for c in range(CHUNKS):
                for copy in early(c, far_ks):
                    copy.start()

    def relay(g):
        f, span, c, size = spans[g]
        if f == 0:
            if c % 2 == 1:
                return
            size = 2
            span = pl.ds(c, size)
        slot = c // 2 if f == 0 else g - len(totals) + CHUNKS // 2
        arrivals = [(0, d - 1, jy, inner_peer(inner - d)) for d in steps_in]
        arrivals += [(1, e - 1, outer_peer(outer - e), ix) for e in steps_out]
        for n, (kind, k, j, i) in enumerate(arrivals):
            drain(ext.at[1 + f, j, i, :, span], hop_recv.at[kind, slot, k])
            if square:
                block, to = (blocks[0], at(*blocks[1])) if n == 0 else (blocks[1], at(*blocks[0]))
                moves = tm > 0 if g in others else tm >= 0

                @pl.when(moves)
                def _():
                    ref = ext.at[1 + f, *block, n, span]
                    remote(ref, ref, relay_send, far_recv.at[min(f, 1)], to).start()

    def own_total(g):
        f, span, _, _ = spans[g]
        total = part[f, :, span, jy, ix]
        if blocks:
            drain(arrived.at[:, f, :, span], rs_recv.at[g])
        for k in range(len(blocks)):
            total = total + arrived[k, f, :, span]
        ext[1 + f, jy, ix, :, span] = total

    def up(c, src, step):
        dst = ext.at[0, jy, ix, :, c]
        return remote(src, dst, z_send, z_recv.at[c], {"tm": tm + step})

    def side(c):
        return remote(ext.at[1, jy, ix, :, c], extra.at[c], z_send, z_recv.at[c], {"tm": tm + 1})

    def send_up(c, src, steps=(2, 1)):
        for step in (k for k in steps if k < steps_tm):
            @pl.when(tm < steps_tm - step)
            def _():
                up(c, src, step).start()

    def early(c, ks):
        ref = ext.at[0, jy, ix, :, c]
        return [remote(ref, ref, early_send, early_recv.at[int(k in far_ks)], at(*blocks[k])) for k in ks]

    def earlier(c):
        @pl.when(jnp.logical_not(even))
        def _():
            up(c, extra.at[c], 1).wait_recv()

        @pl.when(even)
        def _():
            drain(ext.at[pl.ds(0, 2), jy, ix, :, c], z_recv.at[c])
            total = ext[0, jy, ix, :, c] + extra[c]
            ext[0, jy, ix, :, c] = total
            passing[c] = total + ext[1, jy, ix, :, c]
            send_up(c, passing.at[c])

    def share_earlier(c):
        if far_ks:
            @pl.when(first_far)
            def _():
                for copy in early(c, far_ks):
                    copy.start()
        for copy in early(c, near_ks):
            copy.start()

    for g in totals:
        c = spans[g][2]
        own_total(g)

        @pl.when(tm == 0)
        def _():
            send_up(c, ext.at[1, jy, ix, :, c], (2,))
            if c > 0:
                send_up(c - 1, ext.at[1, jy, ix, :, c - 1], (1,))
            if c == CHUNKS - 1:
                send_up(c, ext.at[1, jy, ix, :, c], (1,))

        @pl.when((tm % 2 == 1) & (tm < steps_tm - 1))
        def _():
            side(c).start()

        share(g)
    chunks = list(range(CHUNKS))
    early_planes, last_planes = (tm == 1) | ((tm > 0) & even), (tm > 1) & (tm % 2 == 1)

    def take(planes, n):
        @pl.when(planes)
        def _():
            for c in chunks[n * CHUNKS // len(others):(n + 1) * CHUNKS // len(others)]:
                earlier(c)
                share_earlier(c)

    for n, g in enumerate(others):
        own_total(g)
        share(g)
        take(early_planes, n)
    for g in totals:
        relay(g)
    for n, g in enumerate(others):
        take(last_planes, n)
        if n == len(others) - 1:
            share_last()
        relay(g)

    @pl.when(tm == 0)
    def _():
        ext[0] = jnp.zeros(ext.shape[1:], jnp.float32)

    @pl.when(tm > 0)
    def _():
        if near_ks:
            drain(arrived.at[pl.ds(0, len(near_ks)), 0], early_recv.at[0])

    windows = out.shape[0]
    local = [index[w] - tm * slots for w in range(windows)]
    shares = [[jnp.where(local[w] > t, 1.0, jnp.where(local[w] == t, weight[w], 0.0))
               for t in range(slots)] for w in range(windows)]
    factors = [[share[-1]] + [share[t] - share[-1] for t in range(slots - 1)] for share in shares]

    def blend(j, i, o):
        for w in range(windows):
            total = ext[0, j, i, o] + factors[w][0] * ext[1, j, i, o]
            for t in range(1, slots):
                total = total + factors[w][t] * ext[1 + t, j, i, o]
            out[w, j, i, o] = total

    def blend_over(targets):
        for j, i in targets:
            def step(o, carry):
                blend(j, i, o)
                return carry

            lax.fori_loop(0, 2, step, 0)

    blend_over([(outer_peer(e), inner_peer(d)) for e, d in offsets if e == 0 or d == 0])
    twice = even & (tm < steps_tm - 2)

    @pl.when((tm < steps_tm - 1) & jnp.logical_not(twice))
    def _():
        drain(passing, z_send)

    @pl.when(twice)
    def _():
        drain(ext.at[pl.ds(0, 2), 0, 0], z_send)

    for copy in halos:
        copy.wait_send()
    if blocks:
        drain(arrived, rs_send)
    if near_ks:
        drain(arrived.at[pl.ds(0, len(near_ks))], ag_send)
    if far_ks:
        far = pl.ds(len(near_ks), len(far_ks))
        rest = pl.ds(1, slots - 1)
        if square:
            @pl.when(tm > 0)
            def _():
                drain(ext.at[pl.ds(1, slots), 0, 0], relay_send)

            @pl.when(tm == 0)
            def _():
                drain(ext.at[1, 0, 0], relay_send)
                drain(arrived.at[far, rest], across_send)
        else:
            drain(arrived.at[far], across_send)

    @pl.when(tm > 0)
    def _():
        if blocks:
            drain(arrived.at[:, 0], early_send)

    if far_ks:
        @pl.when(tm > 0)
        def _():
            drain(arrived.at[far, 0], early_recv.at[1])

        drain(arrived.at[far, 0], far_recv.at[0])
        drain(arrived.at[far, rest], far_recv.at[1])
        blend_over([blocks[k] for k in far_ks])


def store(held, out, sem):
    size = held.shape[1] // STORES
    for n in range(STORES):
        span = pl.ds(n * size, size)
        pltpu.make_async_copy(held.at[:, span], out.at[:, span], sem).start()
    drain(held, sem)


def binomial_rings(size):
    column = np.zeros(size)
    column[0] += 1.0 - 4.0 * diffusion
    column[1 % size] += diffusion
    column[-1 % size] += diffusion
    ring = np.stack([np.roll(column, x) for x in range(size)], axis=1)
    return [[math.comb(SMOOTH, k) * diffusion ** k * float(x) for x in np.linalg.matrix_power(ring, SMOOTH - k)[0]]
            for k in range(SMOOTH + 1)]


def pieces_of(slots):
    n = max(CHUNKS // 2, 1)
    return [(0, c, 1) for c in range(CHUNKS)] + [(f, c, n) for f in range(1, slots) for c in range(0, CHUNKS, n)]


def rows_view(x, nx, gy):
    lead = x.shape[:-2]
    x = x.reshape(lead + (nx, gy // LANES, LANES))
    x = jnp.swapaxes(x, -3, -2)
    return x


def per_device(control, vertical_modes, mode_counts, perturbations, slot_index, blend_weight):
    members, slots, levels, nx, gy = perturbations.shape
    modes_n = control.shape[1]
    halves = gy // LANES
    level_rows = nx * halves
    tiles, n_mem, steps_tm = lax.axis_size("tile"), lax.axis_size("mem"), lax.axis_size("tm")
    inner = 2 if n_mem % 2 == 0 else 1
    outer = n_mem // inner
    parts = 2 * CHUNKS
    rows = levels // (n_mem * parts) * level_rows
    assert nx >= SMOOTH and level_rows == 8 and rows % 16 == 0
    norm = 1.0 / math.sqrt(members * n_mem - 1)
    fields = members * modes_n
    c = rows_view(control, nx, gy).reshape(fields, level_rows, LANES)
    q = rows_view(perturbations, nx, gy).reshape(members, slots, outer, inner, 2, CHUNKS, rows, LANES)
    dims = (members, slots, modes_n, nx, halves, outer, inner, rows, tiles, steps_tm, norm)
    f32 = jnp.float32
    n_in, n_out = max(inner - 1, 1), max(outer - 1, 1)
    n_pieces = len(pieces_of(slots))
    sides = 2 if tiles > 2 else 1
    dma = pltpu.SemaphoreType.DMA
    windows = slot_index.shape[0]
    held = pl.pallas_call(
        functools.partial(kernel, dims),
        out_shape=pltpu.VMEM((windows, outer, inner, 2, CHUNKS, rows, LANES), f32),
        in_specs=[
            pl.BlockSpec(memory_space=pltpu.HBM),
            pl.BlockSpec(memory_space=pltpu.HBM),
            pl.BlockSpec(memory_space=pltpu.HBM),
            pl.BlockSpec(memory_space=pltpu.HBM),
            pl.BlockSpec(memory_space=pltpu.HBM),
            pl.BlockSpec(memory_space=pltpu.HBM),
        ],
        out_specs=pl.BlockSpec(memory_space=pltpu.VMEM),
        scratch_shapes=[
            pltpu.VMEM((slots + 1, outer, inner, 2, CHUNKS, rows, LANES), f32),
            pltpu.VMEM((fields, level_rows, LANES), f32),
            pltpu.VMEM((sides, fields, level_rows, LANES), f32),
            pltpu.VMEM((sides, fields, level_rows, LANES), f32),
            pltpu.VMEM(q.shape, q.dtype),
            pltpu.VMEM((fields, level_rows, LANES), f32),
            pltpu.VMEM((slots, 2, CHUNKS, outer, inner, rows, LANES), f32),
            pltpu.VMEM((max(n_mem - 1, 1), slots, 2, CHUNKS, rows, LANES), f32),
            pltpu.VMEM((CHUNKS, 2, rows, LANES), f32),
            pltpu.VMEM((CHUNKS, 2, rows, LANES), f32),
            pltpu.SMEM((modes_n, levels), f32),
            pltpu.SMEM((nx,), jnp.int32),
            pltpu.SMEM((windows,), jnp.int32),
            pltpu.SMEM((windows,), f32),
            dma((5,)),
            dma((n_mem,)),
            dma((sides,)),
            dma((sides,)),
            dma,
            dma((n_pieces,)),
            dma,
            dma((CHUNKS,)),
            dma,
            dma,
            dma,
            dma((2, n_pieces - CHUNKS + CHUNKS // 2, max(n_in, n_out))),
            dma((2,)),
            dma,
            dma((2,)),
            pltpu.SemaphoreType.REGULAR,
        ],
        compiler_params=pltpu.CompilerParams(
            collective_id=0, has_side_effects=True),
    )(c, q, vertical_modes.T, mode_counts, slot_index, blend_weight)
    held = held.reshape(windows, levels * level_rows, LANES)
    out = pl.pallas_call(
        store,
        out_shape=jax.ShapeDtypeStruct((windows, levels * level_rows, LANES), f32),
        in_specs=[pl.BlockSpec(memory_space=pltpu.VMEM)],
        out_specs=pl.BlockSpec(memory_space=pltpu.HBM),
        scratch_shapes=[dma],
        compiler_params=pltpu.CompilerParams(vmem_limit_bytes=8 << 20),
    )(held)
    out = out.reshape(windows, levels, halves, nx, LANES)
    return jnp.swapaxes(out, 2, 3).reshape(windows, levels, nx, gy)


def solution(mesh):
    placed = (
        P("mem", None, "tile", None),
        P(),
        P("tile"),
        P("mem", "tm", None, "tile", None),
        P("tm"),
        P("tm"),
    )
    return jax.shard_map(
        per_device,
        mesh=mesh,
        in_specs=placed,
        out_specs=P("tm", None, "tile", None),
        check_vma=False,
    )
```
